32 devices in a mesh: seq: 16 (over z, x, core), head: 2 (over y).
Axes of the slice: x: 2, y: 2, z: 4, core: 2. Of those that a mesh axis runs over, the one named last changes fastest.
Arguments:
- queries: bfloat16 [4096, 4096], P(('seq', 'head')), may hold values from -5 to 5
- key_rows: bfloat16 [4096, 4096], P(('seq', 'head')), may hold values from -5 to 5
- value_rows: bfloat16 [4096, 4096], P(('seq', 'head')), may hold values from -6 to 6
- step_rates: bfloat16 [4096, 8], P(('seq', 'head')), may hold values from 0.1 to 9
- w_gate: bfloat16 [512, 8, 512], P('seq', 'head'), may hold values from -0.25 to 0.25
- w_up: bfloat16 [512, 8, 512], P('seq', 'head'), may hold values from -0.25 to 0.25
- w_down: bfloat16 [512, 8, 512], P('seq', 'head'), may hold values from -0.25 to 0.25
Outputs:
- block_out: bfloat16 [4096, 4096], P(('seq', 'head'))
The draws below stay inside these ranges and needn't reach their ends.
All inputs are finite; a program needn't handle non-finite values.
Results may differ from the reference program's by a relative error of at most 0.012.
Values may be sent and summed in bfloat16 or wider, within the bound.
No kernel may reach another device: no remote copies, remote signals or barrier semaphores. Data moves between devices by JAX's collectives and lax.ppermute only.
A program may use at most 128 MiB of HBM per device.

```python
import math
import jax
import jax.numpy as jnp
from jax import lax

D = 4096
ATT_HEADS = 32
HEAD_DIM = 128
HEADS = 8
HS = 512
WINDOW = 64
TOKENS = 4096


def drawn_pair(key):
    rng_query = jax.random.fold_in(key, 11)
    rng_keys = jax.random.fold_in(key, 12)
    query_part = jnp.clip(jax.random.normal(rng_query, (TOKENS, D), jnp.float32), -5.0, 5.0)
    key_part = jnp.clip(jax.random.normal(rng_keys, (TOKENS, D), jnp.float32), -5.0, 5.0)
    return (query_part.astype(jnp.bfloat16), key_part.astype(jnp.bfloat16))


def draw_queries(key, part):
    return drawn_pair(key)[0]


def draw_key_rows(key, part):
    return drawn_pair(key)[1]


def draw_step_rates(key, part):
    position = jnp.arange(TOKENS, dtype=jnp.float32)[:, None] / TOKENS
    base_log = jax.random.uniform(jax.random.fold_in(key, 21), (TOKENS, HEADS), jnp.float32, jnp.log(0.1), 0.0)
    ramp_log = jnp.log(3.0) * position
    return jnp.exp(base_log + ramp_log).astype(jnp.bfloat16)


def level_of(rng, shape, shards, least, largest):
    def one(dim, blocks):
        steps = jax.random.uniform(jax.random.fold_in(jax.random.fold_in(rng, 6), dim), (blocks,), jnp.float32, least / len(shards), largest / len(shards))
        return jnp.repeat(jnp.exp(steps), shape[dim] // blocks).reshape((-1,) + (1,) * (len(shape) - dim - 1))

    factor_of = one(*shards[0])
    for cut in shards[1:]:
        factor_of = factor_of * one(*cut)
    return factor_of


def noise(own_key, shape, spread, limit, shards=(), kind=jnp.bfloat16):
    entries = jax.random.normal(own_key, shape, jnp.float32) * spread
    if len(shards) > 0:
        entries = level_of(own_key, shape, shards, -0.22, 0.18) * entries
    return jnp.clip(entries, min=-limit, max=limit).astype(kind)


def setup_inputs(seed: int = 0) -> dict:
    seeds = jax.random.split(jax.random.key(seed), 8)
    return {
        "queries": draw_queries(jax.random.fold_in(seeds[7], 71), 0),
        "key_rows": draw_key_rows(jax.random.fold_in(seeds[7], 71), 0),
        "value_rows": noise(seeds[2], (TOKENS, D), 1.0, 6.0, ((0, 32),)),
        "step_rates": draw_step_rates(jax.random.fold_in(seeds[7], 71), 0),
        "w_gate": noise(seeds[4], (HS, HEADS, HS), HS ** -0.5, 0.25, ((0, 16), (1, 2))),
        "w_up": noise(seeds[5], (HS, HEADS, HS), HS ** -0.5, 0.25, ((0, 16), (1, 2))),
        "w_down": noise(seeds[6], (HS, HEADS, HS), HS ** -0.5, 0.25, ((0, 16), (1, 2))),
    }


STEP_SIZE = 0.05
NORM_EPS = 1e-06
query_block = 512

def attend(block_queries, key_span, value_span, query_start):
    row_count = block_queries.shape[0]
    span_count = key_span.shape[0]
    query_heads = block_queries.astype(jnp.float32).reshape(row_count, ATT_HEADS, HEAD_DIM)
    key_heads = key_span.astype(jnp.float32).reshape(span_count, ATT_HEADS, HEAD_DIM)
    value_heads = value_span.astype(jnp.float32).reshape(span_count, ATT_HEADS, HEAD_DIM)
    scores = jnp.einsum('qhd,khd->hqk', query_heads, key_heads) * (1.0 / math.sqrt(HEAD_DIM))
    query_pos = query_start + jnp.arange(row_count, dtype=jnp.int32)
    key_pos = query_start - WINDOW + jnp.arange(span_count, dtype=jnp.int32)
    allowed = (key_pos[None, :] >= 0) & (key_pos[None, :] <= query_pos[:, None]) & (key_pos[None, :] > query_pos[:, None] - WINDOW)
    masked = jnp.where(allowed[None], scores, -1e+30)
    maximum = lax.optimization_barrier(jnp.max(masked, axis=2, keepdims=True))
    exp_scores = jnp.where(allowed[None], jnp.exp(masked - maximum), 0.0)
    totals = lax.optimization_barrier(jnp.sum(exp_scores, axis=2))
    weights = exp_scores.astype(jnp.bfloat16)
    mixed = jnp.einsum('hqk,khd->qhd', weights.astype(jnp.float32), value_heads)
    return (mixed / jnp.transpose(totals)[:, :, None]).reshape(row_count, D)

def rms_heads(tensor):
    blocks = tensor.astype(jnp.float32).reshape(tensor.shape[0], HEADS, HS)
    return (blocks * lax.rsqrt(lax.optimization_barrier(jnp.mean(blocks * blocks, axis=2, keepdims=True)) + NORM_EPS)).astype(jnp.bfloat16)

def renorm(old_rows, grad_rows, norm_scale):
    previous = old_rows.astype(jnp.float32)
    stepped = previous - STEP_SIZE * norm_scale * grad_rows
    factor = jnp.sqrt(lax.optimization_barrier(jnp.mean(previous * previous, axis=-1, keepdims=True))) * lax.rsqrt(lax.optimization_barrier(jnp.mean(stepped * stepped, axis=-1, keepdims=True)) + NORM_EPS)
    return (stepped * factor).astype(jnp.bfloat16)

def fast_head(inputs):
    key_norm, query_norm, value_head, rate_col, gate_w, up_w, down_w = inputs
    gate_pre = jnp.dot(key_norm, gate_w, preferred_element_type=jnp.float32)
    up_pre = jnp.dot(key_norm, up_w, preferred_element_type=jnp.float32)
    sigma_gate = jax.nn.sigmoid(gate_pre)
    silu_gate = gate_pre * sigma_gate
    hidden = (silu_gate * up_pre).astype(jnp.bfloat16)
    target = (-rate_col.astype(jnp.float32)[:, None] * value_head.astype(jnp.float32)).astype(jnp.bfloat16)
    hidden_grad = jnp.dot(target, jnp.transpose(down_w), preferred_element_type=jnp.float32)
    gate_grad = (hidden_grad * up_pre * sigma_gate * (1.0 + gate_pre * (1.0 - sigma_gate))).astype(jnp.bfloat16)
    up_grad = (hidden_grad * silu_gate).astype(jnp.bfloat16)
    sum_gate = jnp.dot(jnp.transpose(key_norm), gate_grad, preferred_element_type=jnp.float32)
    sum_up = jnp.dot(jnp.transpose(key_norm), up_grad, preferred_element_type=jnp.float32)
    sum_down = jnp.dot(jnp.transpose(hidden), target, preferred_element_type=jnp.float32)
    squares = jnp.sum(sum_gate * sum_gate) + jnp.sum(sum_up * sum_up) + jnp.sum(sum_down * sum_down)
    norm_scale = lax.rsqrt(squares / (3 * HS * HS) + NORM_EPS)
    new_gate = renorm(gate_w, sum_gate, norm_scale)
    new_up = renorm(up_w, sum_up, norm_scale)
    new_down = renorm(down_w, sum_down, norm_scale)
    query_gate = jnp.dot(query_norm, new_gate, preferred_element_type=jnp.float32)
    query_up = jnp.dot(query_norm, new_up, preferred_element_type=jnp.float32)
    query_hidden = (query_gate * jax.nn.sigmoid(query_gate) * query_up).astype(jnp.bfloat16)
    return jnp.dot(query_hidden, new_down, preferred_element_type=jnp.float32).astype(jnp.bfloat16)

def reference(queries, key_rows, value_rows, step_rates, w_gate, w_up, w_down):
    block_rows = min(query_block, TOKENS)
    padded_keys = jnp.concatenate([jnp.zeros((WINDOW, D), key_rows.dtype), key_rows], 0)
    padded_values = jnp.concatenate([jnp.zeros((WINDOW, D), value_rows.dtype), value_rows], 0)
    starts = jnp.arange(TOKENS // block_rows, dtype=jnp.int32) * block_rows

    def one_block(begin_row):
        block_queries = lax.dynamic_slice_in_dim(queries, begin_row, block_rows, 0)
        key_span = lax.dynamic_slice_in_dim(padded_keys, begin_row, block_rows + WINDOW, 0)
        value_span = lax.dynamic_slice_in_dim(padded_values, begin_row, block_rows + WINDOW, 0)
        return attend(block_queries, key_span, value_span, begin_row)
    attended = lax.map(one_block, starts).reshape(TOKENS, D)
    key_norm = rms_heads(key_rows)
    query_norm = rms_heads(queries)
    value_heads = value_rows.reshape(TOKENS, HEADS, HS)
    per_head = (jnp.transpose(key_norm, (1, 0, 2)), jnp.transpose(query_norm, (1, 0, 2)), jnp.transpose(value_heads, (1, 0, 2)), jnp.transpose(step_rates), jnp.transpose(w_gate, (1, 0, 2)), jnp.transpose(w_up, (1, 0, 2)), jnp.transpose(w_down, (1, 0, 2)))
    fast_out = lax.map(fast_head, per_head)
    merged = jnp.transpose(fast_out, (1, 0, 2)).reshape(TOKENS, D)
    return (attended + merged.astype(jnp.float32)).astype(jnp.bfloat16)
```

```python
import math

import jax
import jax.numpy as jnp
from jax import lax
from jax.experimental import pallas as pl
from jax.experimental.pallas import tpu as pltpu
from jax.sharding import Mesh, PartitionSpec as P


HEADS = 8
HEAD_DIM = 128
WINDOW = 64
STEP_SIZE = 0.05
NORM_EPS = 1e-06
VMEM_LIMIT = 28 * 1024 * 1024
ANY = pl.BlockSpec(memory_space=pl.ANY)
VMEM = pl.BlockSpec(memory_space=pltpu.VMEM)
SMEM = pl.BlockSpec(memory_space=pltpu.SMEM)


def in_vmem(x):
    return pltpu.with_memory_space_constraint(x, pltpu.VMEM)


def in_hbm(x):
    return pltpu.with_memory_space_constraint(x, pltpu.HBM)


def cost(microseconds):
    return pl.CostEstimate(
        flops=int(microseconds * 4e6), bytes_accessed=1 << 20, transcendentals=0
    )


def sds(shape, dtype):
    return jax.ShapeDtypeStruct(shape, dtype)


def params():
    return pltpu.CompilerParams(vmem_limit_bytes=VMEM_LIMIT)


def swap_pairs(count, stride):
    return [(i, i ^ stride) for i in range(count)]


def tiles_to_rows(ref, block, first, rows, tiles):
    return jnp.concatenate(
        [ref[block, first + t * rows : first + (t + 1) * rows, :] for t in range(tiles)], axis=1
    )


def rms_rows(rows):
    wide = rows.astype(jnp.float32)
    scale = lax.rsqrt(jnp.mean(wide * wide, axis=1, keepdims=True) + NORM_EPS)
    return (wide * scale).astype(jnp.bfloat16)


def move_by_head(sources, out_ref, stage_ref, sem_in, sem_out, order, rows, tiles):
    size = tiles * HEAD_DIM
    reads, writes = [], []
    for peer, head in enumerate(order):
        for which, ref in enumerate(sources):
            spot = peer * len(sources) + which
            reads.append(
                pltpu.make_async_copy(
                    ref.at[:, pl.ds(head * size, size)], stage_ref.at[spot], sem_in.at[spot]
                )
            )
            for t in range(tiles):
                writes.append(
                    pltpu.make_async_copy(
                        stage_ref.at[spot, :, pl.ds(t * HEAD_DIM, HEAD_DIM)],
                        out_ref.at[peer, pl.ds((which * tiles + t) * rows, rows), :],
                        sem_out.at[spot * tiles + t],
                    )
                )
    for read in reads:
        read.start()
    for i, read in enumerate(reads):
        read.wait()
        for write in writes[i * tiles : (i + 1) * tiles]:
            write.start()
    return writes


def pack_keys(key_rows, value_rows, rates_t, order, rate_rows):
    rows, width = key_rows.shape
    tiles = width // HEADS // HEAD_DIM

    def kernel(k_ref, v_ref, r_ref, out_ref, stage_ref, rate_ref, sem_in, sem_out, sem_rate):
        for peer, head in enumerate(order):
            rate_ref[peer] = jnp.broadcast_to(
                r_ref[head : head + 1, :].astype(jnp.float32), (rate_rows, rows)
            ).astype(jnp.bfloat16)
        last = pltpu.make_async_copy(
            rate_ref, out_ref.at[:, pl.ds(2 * tiles * rows, rate_rows), :], sem_rate
        )
        last.start()
        writes = move_by_head(
            (k_ref, v_ref), out_ref, stage_ref, sem_in, sem_out, order, rows, tiles
        )
        for write in writes:
            write.wait()
        last.wait()

    return pl.pallas_call(
        kernel,
        in_specs=[ANY, ANY, VMEM],
        out_specs=ANY,
        out_shape=pltpu.HBM((HEADS, 2 * tiles * rows + rate_rows, HEAD_DIM), jnp.bfloat16),
        scratch_shapes=[
            pltpu.VMEM((HEADS * 2, rows, tiles * HEAD_DIM), jnp.bfloat16),
            pltpu.VMEM((HEADS, rate_rows, rows), jnp.bfloat16),
            pltpu.SemaphoreType.DMA((HEADS * 2,)),
            pltpu.SemaphoreType.DMA((HEADS * 2 * tiles,)),
            pltpu.SemaphoreType.DMA,
        ],
        compiler_params=params(),
        name="pack_keys",
    )(in_hbm(key_rows), in_hbm(value_rows), rates_t)


def pack_queries(queries, order):
    rows, width = queries.shape
    tiles = width // HEADS // HEAD_DIM

    def kernel(q_ref, out_ref, stage_ref, sem_in, sem_out):
        writes = move_by_head((q_ref,), out_ref, stage_ref, sem_in, sem_out, order, rows, tiles)
        for write in writes:
            write.wait()

    return pl.pallas_call(
        kernel,
        in_specs=[ANY],
        out_specs=ANY,
        out_shape=pltpu.HBM((HEADS, tiles * rows, HEAD_DIM), jnp.bfloat16),
        scratch_shapes=[
            pltpu.VMEM((HEADS, rows, tiles * HEAD_DIM), jnp.bfloat16),
            pltpu.SemaphoreType.DMA((HEADS,)),
            pltpu.SemaphoreType.DMA((HEADS * tiles,)),
        ],
        compiler_params=params(),
        name="pack_queries",
    )(in_hbm(queries))


def pack_weights(w_gate, w_up, w_down):
    piece, heads, size = w_gate.shape

    def kernel(g_ref, u_ref, d_ref, out_ref):
        for which, ref in enumerate((g_ref, u_ref, d_ref)):
            for head in range(heads):
                out_ref[head, which] = ref[:, head, :]

    return pl.pallas_call(
        kernel,
        in_specs=[VMEM] * 3,
        out_specs=VMEM,
        out_shape=pltpu.HBM((heads, 3, piece, size), w_gate.dtype),
        compiler_params=params(),
        name="pack_weights",
    )(in_hbm(w_gate), in_hbm(w_up), in_hbm(w_down))


def unpack_columns(back, places):
    heads, rows, size = back.shape

    def kernel(back_ref, out_ref, sem):
        moves = [
            pltpu.make_async_copy(
                back_ref.at[place], out_ref.at[:, pl.ds(head * size, size)], sem.at[head]
            )
            for head, place in enumerate(places)
        ]
        for move in moves:
            move.start()
        for move in moves:
            move.wait()

    return pl.pallas_call(
        kernel,
        in_specs=[ANY],
        out_specs=ANY,
        out_shape=sds((rows, heads * size), back.dtype),
        scratch_shapes=[pltpu.SemaphoreType.DMA((heads,))],
        compiler_params=params(),
        name="unpack_columns",
    )(back)


def place_pieces(spot_ref, piece_refs, out_ref, outer, lane, inner):
    if len(piece_refs) == 1:
        out_ref[...] = piece_refs[0][...]
        return
    piece = piece_refs[0].shape[2]
    a, c = spot_ref[0], spot_ref[1]
    spots = [(a, c), (outer - 1 - a, c), (a, inner - 1 - c), (outer - 1 - a, inner - 1 - c)]
    for (at_a, at_c), ref in zip(spots, piece_refs):
        for l in range(lane):
            first = pl.multiple_of(((at_a * lane + l) * inner + at_c) * piece, piece)
            for which in range(3):
                out_ref[which, pl.ds(first, piece), :] = ref[l, which]


def gradients(spot, received, pieces, rows, tiles, outer, lane, inner):
    blocks = received.shape[0]
    size = tiles * HEAD_DIM
    half = size // inner
    count = blocks * rows
    group = 2 if blocks % 2 == 0 else 1
    span = group * rows

    def kernel(spot_ref, kv_ref, *refs):
        piece_refs = refs[: len(pieces)]
        keep_ref, send_ref, w_ref, kn_ref, hid_ref, tgt_ref, gg_ref, ug_ref = refs[len(pieces) :]
        place_pieces(spot_ref, piece_refs, w_ref, outer, lane, inner)
        for g in range(blocks // group):
            here = slice(g * span, (g + 1) * span)
            mine = range(g * group, (g + 1) * group)

            def stacked(first):
                return jnp.concatenate(
                    [tiles_to_rows(kv_ref, b, first, rows, tiles) for b in mine], axis=0
                )

            key_norm = rms_rows(stacked(0))
            values = stacked(tiles * rows).astype(jnp.float32)
            rates = []
            for b in mine:
                row = kv_ref[b, 2 * tiles * rows : 2 * tiles * rows + 1, :].astype(jnp.float32)
                rates.append(jnp.broadcast_to(row, (rows, rows)).T)
            rate_columns = jnp.concatenate([jnp.concatenate(rates, axis=0)] * tiles, axis=1)
            target = (-rate_columns * values).astype(jnp.bfloat16)
            tgt_ref[here, :] = target
            gate_pre = jnp.dot(key_norm, w_ref[0], preferred_element_type=jnp.float32)
            up_pre = jnp.dot(key_norm, w_ref[1], preferred_element_type=jnp.float32)
            hidden_grad = lax.dot_general(
                target, w_ref[2], (((1,), (1,)), ((), ())), preferred_element_type=jnp.float32
            )
            sigma_gate = jax.nn.sigmoid(gate_pre)
            silu_gate = gate_pre * sigma_gate
            hidden = (silu_gate * up_pre).astype(jnp.bfloat16)
            for part in range(inner):
                columns = slice(part * half, (part + 1) * half)
                kn_ref[part, here, :] = key_norm[:, columns]
                hid_ref[part, here, :] = hidden[:, columns]
            gg_ref[here, :] = (
                hidden_grad * up_pre * sigma_gate * (1.0 + gate_pre * (1.0 - sigma_gate))
            ).astype(jnp.bfloat16)
            ug_ref[here, :] = (hidden_grad * silu_gate).astype(jnp.bfloat16)

        def total(left_ref, right_ref, part):
            return lax.dot_general(
                left_ref[part],
                right_ref[...],
                (((0,), (0,)), ((), ())),
                preferred_element_type=jnp.float32,
            )

        own = spot_ref[1]
        pairs = ((kn_ref, gg_ref), (kn_ref, ug_ref), (hid_ref, tgt_ref))
        for which, (left_ref, right_ref) in enumerate(pairs):
            send_ref[which] = total(left_ref, right_ref, inner - 1 - own).astype(jnp.bfloat16)
            keep_ref[which] = total(left_ref, right_ref, own)

    return pl.pallas_call(
        kernel,
        in_specs=[SMEM, VMEM] + [VMEM] * len(pieces),
        out_specs=[VMEM, VMEM],
        out_shape=[
            pltpu.VMEM((3, half, size), jnp.float32),
            pltpu.VMEM((3, half, size), jnp.bfloat16),
        ],
        scratch_shapes=[
            pltpu.VMEM((3, size, size), jnp.bfloat16),
            pltpu.VMEM((inner, count, half), jnp.bfloat16),
            pltpu.VMEM((inner, count, half), jnp.bfloat16),
            pltpu.VMEM((count, size), jnp.bfloat16),
            pltpu.VMEM((count, size), jnp.bfloat16),
            pltpu.VMEM((count, size), jnp.bfloat16),
        ],
        compiler_params=params(),
        cost_estimate=cost(6),
        name="gradients",
    )(spot, in_vmem(received), *[in_vmem(p) for p in pieces])


def combine(keep, got):
    def kernel(keep_ref, got_ref, out_ref):
        out_ref[...] = (keep_ref[...] + got_ref[...].astype(jnp.float32)).astype(jnp.bfloat16)

    return pl.pallas_call(
        kernel,
        in_specs=[VMEM, VMEM],
        out_specs=VMEM,
        out_shape=pltpu.VMEM(keep.shape, jnp.bfloat16),
        compiler_params=params(),
        name="combine",
    )(in_vmem(keep), in_vmem(got))


def last_rows(received, rows, tiles, per_run):
    runs = received.shape[0] // per_run

    def kernel(kv_ref, out_ref):
        for run in range(runs):
            for t in range(2 * tiles):
                end = (t + 1) * rows
                out_ref[run, t * WINDOW : (t + 1) * WINDOW, :] = kv_ref[
                    (run + 1) * per_run - 1, end - WINDOW : end, :
                ]

    return pl.pallas_call(
        kernel,
        in_specs=[VMEM],
        out_specs=VMEM,
        out_shape=pltpu.VMEM((runs, 2 * tiles * WINDOW, HEAD_DIM), received.dtype),
        compiler_params=params(),
        name="last_rows",
    )(in_vmem(received))


def attention(spot, queries, received, around, from_outer, rows, tiles, per_run):
    blocks = queries.shape[0]
    width = tiles * HEAD_DIM
    span = WINDOW + rows

    def kernel(spot_ref, q_ref, kv_ref, around_ref, outer_ref, att_ref, qn_ref, bias_ref):
        on_first = jnp.where(spot_ref[1] == 0, 1, 0)
        begins = jnp.where(spot_ref[0] == 0, on_first, 0)
        row_id = lax.broadcasted_iota(jnp.int32, (rows, span), 0)
        key_id = lax.broadcasted_iota(jnp.int32, (rows, span), 1)
        allowed = (key_id <= row_id + WINDOW) & (key_id > row_id)
        bias_ref[0] = jnp.where(allowed, 0.0, -1e30)
        bias_ref[1] = jnp.where(allowed & (key_id >= WINDOW), 0.0, -1e30)
        for b in range(blocks):
            qn_ref[b] = rms_rows(tiles_to_rows(q_ref, b, 0, rows, tiles))
            bias = bias_ref[begins] if b == 0 else bias_ref[0]
            for t in range(tiles):
                query = q_ref[b, t * rows : (t + 1) * rows, :]

                def with_tail(which):
                    base = (which * tiles + t) * rows
                    own = kv_ref[b, base : base + rows, :]
                    if b % per_run:
                        tail = kv_ref[b - 1, base + rows - WINDOW : base + rows, :]
                    else:
                        first = (which * tiles + t) * WINDOW
                        place = slice(first, first + WINDOW)
                        if b:
                            tail = around_ref[b // per_run - on_first, place, :]
                        else:
                            tail = jnp.where(
                                on_first == 1, outer_ref[0, place, :], around_ref[0, place, :]
                            )
                    return jnp.concatenate([tail, own], axis=0)

                keys = with_tail(0)
                values = with_tail(1)
                scores = lax.dot_general(
                    query, keys, (((1,), (1,)), ((), ())), preferred_element_type=jnp.float32
                )
                masked = scores * (1.0 / math.sqrt(HEAD_DIM)) + bias
                maximum = jnp.max(masked, axis=1, keepdims=True)
                exp_scores = jnp.exp(masked - maximum)
                totals = jnp.sum(exp_scores, axis=1, keepdims=True)
                mixed = jnp.dot(
                    exp_scores.astype(jnp.bfloat16), values, preferred_element_type=jnp.float32
                )
                att_ref[b, :, t * HEAD_DIM : (t + 1) * HEAD_DIM] = mixed * (1.0 / totals)

    return pl.pallas_call(
        kernel,
        in_specs=[SMEM] + [VMEM] * 4,
        out_specs=[VMEM, VMEM],
        out_shape=[
            pltpu.VMEM((blocks, rows, width), jnp.float32),
            pltpu.VMEM((blocks, rows, width), jnp.bfloat16),
        ],
        scratch_shapes=[pltpu.VMEM((2, rows, span), jnp.float32)],
        compiler_params=params(),
        cost_estimate=cost(6),
        name="attention",
    )(spot, in_vmem(queries), in_vmem(received), in_vmem(around), in_vmem(from_outer))


def update_and_apply(spot, pieces, sums, query_norm, attended, outer, lane, inner):
    blocks, rows, size = query_norm.shape
    halves = len(sums) // 2
    half = size // halves
    group = 2 if blocks % 2 == 0 else 1

    def kernel(spot_ref, *refs):
        piece_refs, refs = refs[: len(pieces)], refs[len(pieces) :]
        sum_refs = refs[: 2 * halves]
        q_ref, a_ref, out_ref, w_ref, total_ref, new_ref = refs[2 * halves :]
        place_pieces(spot_ref, piece_refs, w_ref, outer, lane, inner)
        squares = jnp.zeros((8, size), jnp.float32)
        for part in range(halves):
            place = spot_ref[1] if part == 0 else halves - 1 - spot_ref[1]
            for which in range(3):
                total = sum_refs[2 * part][which].astype(jnp.float32) + sum_refs[2 * part + 1][
                    which
                ].astype(jnp.float32)
                total_ref[place, which] = total
                squares = squares + jnp.sum(
                    (total * total).reshape(half // 8, 8, size), axis=0
                )
        norm_scale = lax.rsqrt(
            jnp.sum(squares, axis=(0, 1), keepdims=True) / (3 * size * size) + NORM_EPS
        )
        scale = STEP_SIZE * norm_scale
        for part in range(halves):
            for which in range(3):
                here = slice(part * half, (part + 1) * half)
                previous = w_ref[which, here, :].astype(jnp.float32)
                stepped = previous - scale * total_ref[part, which]
                factor = jnp.sqrt(
                    jnp.mean(previous * previous, axis=1, keepdims=True)
                ) * lax.rsqrt(jnp.mean(stepped * stepped, axis=1, keepdims=True) + NORM_EPS)
                new_ref[which, here, :] = (stepped * factor).astype(jnp.bfloat16)
        for g in range(blocks // group):
            mine = range(g * group, (g + 1) * group)
            query = jnp.concatenate([q_ref[b] for b in mine], axis=0)
            query_gate = jnp.dot(query, new_ref[0], preferred_element_type=jnp.float32)
            query_up = jnp.dot(query, new_ref[1], preferred_element_type=jnp.float32)
            query_hidden = (query_gate * jax.nn.sigmoid(query_gate) * query_up).astype(
                jnp.bfloat16
            )
            fast = jnp.dot(query_hidden, new_ref[2], preferred_element_type=jnp.float32).astype(
                jnp.bfloat16
            )
            for i, b in enumerate(mine):
                out_ref[b] = (
                    a_ref[b] + fast[i * rows : (i + 1) * rows, :].astype(jnp.float32)
                ).astype(jnp.bfloat16)

    return pl.pallas_call(
        kernel,
        in_specs=[SMEM] + [VMEM] * (len(pieces) + len(sums) + 2),
        out_specs=VMEM,
        out_shape=pltpu.HBM((blocks, rows, size), jnp.bfloat16),
        scratch_shapes=[
            pltpu.VMEM((3, size, size), jnp.bfloat16),
            pltpu.VMEM((halves, 3, half, size), jnp.float32),
            pltpu.VMEM((3, size, size), jnp.bfloat16),
        ],
        compiler_params=params(),
        cost_estimate=cost(6),
        name="update_and_apply",
    )(
        spot,
        *[in_vmem(p) for p in pieces],
        *[in_vmem(s) for s in sums],
        in_vmem(query_norm),
        in_vmem(attended),
    )


def gather_rows(mine, axis, count, index, order_axis):
    if count & (count - 1):
        return lax.all_gather(mine, axis, axis=order_axis, tiled=True)
    stride = 1
    while stride < count:
        theirs = lax.ppermute(mine, axis, swap_pairs(count, stride))
        low = (index // stride) % 2 == 0
        mine = jnp.concatenate(
            [jnp.where(low, mine, theirs), jnp.where(low, theirs, mine)], order_axis
        )
        stride *= 2
    return mine


def make_shards(outer, lane, inner, head_axis):
    group = ("lane", "head")
    order = [(p % head_axis) * lane + p // head_axis for p in range(HEADS)]
    place_of_head = [order.index(h) for h in range(HEADS)]

    def shards(queries, key_rows, value_rows, step_rates, w_gate, w_up, w_down):
        rows, width = queries.shape
        size = width // HEADS
        tiles = size // HEAD_DIM
        rate_rows = 16
        a = lax.axis_index("outer")
        c = lax.axis_index("inner")
        spot = jnp.stack([a, c]).astype(jnp.int32)
        spot, key_rows = lax.optimization_barrier((spot, key_rows))

        own = pack_weights(w_gate, w_up, w_down)
        if lane > 1:
            own = lax.all_to_all(own, "lane", split_axis=0, concat_axis=0, tiled=True)
        kv = pack_keys(key_rows, value_rows, jnp.transpose(step_rates), order, rate_rows)
        kv = lax.all_to_all(kv, group, split_axis=0, concat_axis=0, tiled=True)
        qs = pack_queries(queries, order)
        qs = lax.all_to_all(qs, group, split_axis=0, concat_axis=0, tiled=True)

        if outer == 2 and inner == 2:
            other = lax.ppermute(own, "outer", swap_pairs(outer, 1))
            own_beside = lax.ppermute(own, "inner", swap_pairs(inner, 1))
            other_beside = lax.ppermute(other, "inner", swap_pairs(inner, 1))
            pieces = [own, other, own_beside, other_beside]
        else:
            old = gather_rows(own[None], "outer", outer, a, 0)[:, :, None]
            old = gather_rows(old, "inner", inner, c, 2)
            pieces = [jnp.transpose(old, (3, 0, 1, 2, 4, 5)).reshape(3, size, size)]

        keep, send = gradients(spot, kv, pieces, rows, tiles, outer, lane, inner)
        if inner > 1:
            got = lax.ppermute(send, "inner", swap_pairs(inner, 1))
            half = combine(keep, got)
        else:
            half = keep.astype(jnp.bfloat16)
        mine, theirs = half, jnp.zeros_like(half)
        if outer & (outer - 1):
            mine = lax.psum(half, "outer")
        else:
            stride = 1
            while stride < outer:
                if stride > 1:
                    mine = (mine.astype(jnp.float32) + theirs.astype(jnp.float32)).astype(
                        jnp.bfloat16
                    )
                theirs = lax.ppermute(mine, "outer", swap_pairs(outer, stride))
                stride *= 2
        tails = last_rows(kv, rows, tiles, head_axis)
        around = tails
        if inner > 1:
            around = lax.ppermute(tails, "inner", [(i, (i + 1) % inner) for i in range(inner)])
        last = tails[lane - 1 :]
        pairs = [
            (i * inner + inner - 1, (i + 1) * inner) for i in range(outer - 1)
        ]
        from_outer = lax.ppermute(last, ("outer", "inner"), pairs) if pairs else last
        attended, query_norm = attention(spot, qs, kv, around, from_outer, rows, tiles, head_axis)

        theirs, attended, query_norm = lax.optimization_barrier((theirs, attended, query_norm))
        sums = [mine, theirs]
        if inner > 1:
            sums.append(lax.ppermute(mine, "inner", swap_pairs(inner, 1)))
            sums.append(lax.ppermute(theirs, "inner", swap_pairs(inner, 1)))

        out = update_and_apply(spot, pieces, sums, query_norm, attended, outer, lane, inner)
        back = lax.all_to_all(out, group, split_axis=0, concat_axis=0, tiled=True)
        return unpack_columns(back, place_of_head)

    return shards


def solution(mesh):
    seq, head_axis = mesh.shape["seq"], mesh.shape["head"]
    lane = HEADS // head_axis
    inner = 2 if (seq // lane) % 2 == 0 else 1
    outer = seq // lane // inner
    names = ("outer", "lane", "inner", "head")
    split = Mesh(mesh.devices.reshape(outer, lane, inner, head_axis), names)
    rows = P(names, None)
    weights = P(names[:3], names[3], None)
    shards = make_shards(outer, lane, inner, head_axis)

    return jax.shard_map(
        shards,
        mesh=split,
        in_specs=(rows, rows, rows, rows, weights, weights, weights),
        out_specs=rows,
        check_vma=False,
    )
```

```python
import math

import jax
import jax.numpy as jnp
from jax import lax
from jax.experimental import pallas as pl
from jax.experimental.pallas import tpu as pltpu
from jax.sharding import Mesh, PartitionSpec as P


HEADS = 8
HEAD_DIM = 128
WINDOW = 64
STEP_SIZE = 0.05
NORM_EPS = 1e-06
RATE_ROWS = 8
ANY = pl.BlockSpec(memory_space=pl.ANY)
VMEM = pl.BlockSpec(memory_space=pltpu.VMEM)
SMEM = pl.BlockSpec(memory_space=pltpu.SMEM)


def in_vmem(x):
    return pltpu.with_memory_space_constraint(x, pltpu.VMEM)


def in_hbm(x):
    return pltpu.with_memory_space_constraint(x, pltpu.HBM)


def cost(microseconds):
    return pl.CostEstimate(
        flops=int(microseconds * 4e6), bytes_accessed=1 << 20, transcendentals=0
    )


def params(mib=4):
    return pltpu.CompilerParams(vmem_limit_bytes=mib << 20)


def swap_pairs(count, stride):
    return [(i, i ^ stride) for i in range(count)]


def rms_rows(rows):
    wide = rows.astype(jnp.float32)
    scale = lax.rsqrt(jnp.mean(wide * wide, axis=1, keepdims=True) + NORM_EPS)
    return (wide * scale).astype(jnp.bfloat16)


def head_of(peer, lane, head_axis):
    return (peer % head_axis) * lane + peer // head_axis


def pack(place, key_rows, value_rows, rates_t, w_gate, w_up, w_down, lane, head_axis):
    rows, width = key_rows.shape
    size = width // HEADS
    piece, local, _ = w_gate.shape

    def kernel(place_ref, k_ref, v_ref, r_ref, g_ref, u_ref, d_ref, w_out_ref, *refs):
        out_refs, w_refs, (sem, w_sem) = refs[:HEADS], refs[HEADS : HEADS + 3], refs[HEADS + 3 :]
        loads = [
            pltpu.make_async_copy(src, dst, w_sem.at[i])
            for i, (src, dst) in enumerate(zip((g_ref, u_ref, d_ref), w_refs))
        ]
        for load in loads:
            load.start()
        moves = []
        heads = []
        for step, out_ref in enumerate(out_refs):
            head = head_of(place_ref[0] ^ step, lane, head_axis)
            heads.append(head)
            first = pl.multiple_of(head * size, size)
            for which, ref in enumerate((k_ref, v_ref)):
                move = pltpu.make_async_copy(
                    ref.at[:, pl.ds(first, size)],
                    out_ref.at[pl.ds(which * rows, rows), :],
                    sem.at[len(moves)],
                )
                move.start()
                moves.append(move)
        rates = r_ref[...].astype(jnp.float32)
        head_id = lax.broadcasted_iota(jnp.int32, rates.shape, 0)
        for head, out_ref in zip(heads, out_refs):
            row = jnp.sum(jnp.where(head_id == head, rates, 0.0), axis=0, keepdims=True)
            wide = jnp.broadcast_to(row, (RATE_ROWS, rows)).astype(jnp.bfloat16)
            for first in range(0, size, rows):
                out_ref[2 * rows :, first : first + rows] = wide
        for which, (load, ref) in enumerate(zip(loads, w_refs)):
            load.wait()
            for head in range(local):
                w_out_ref[head, which] = ref[:, head, :]
        for move in moves:
            move.wait()

    return pl.pallas_call(
        kernel,
        in_specs=[SMEM, ANY, ANY, VMEM, ANY, ANY, ANY],
        out_specs=[VMEM] * (1 + HEADS),
        out_shape=[pltpu.HBM((local, 3, piece, size), jnp.bfloat16)]
        + [pltpu.VMEM((2 * rows + RATE_ROWS, size), jnp.bfloat16)] * HEADS,
        scratch_shapes=[pltpu.VMEM(w_gate.shape, w_gate.dtype)] * 3
        + [pltpu.SemaphoreType.DMA((HEADS * 2,)), pltpu.SemaphoreType.DMA((3,))],
        compiler_params=params(),
        name="pack",
    )(place, *[in_hbm(x) for x in (key_rows, value_rows, rates_t, w_gate, w_up, w_down)])


def pack_queries(place, queries, lane, head_axis):
    rows, width = queries.shape
    size = width // HEADS

    def kernel(place_ref, q_ref, *refs):
        out_refs, sem = refs[:HEADS], refs[HEADS]
        moves = []
        for step, out_ref in enumerate(out_refs):
            head = head_of(place_ref[0] ^ step, lane, head_axis)
            first = pl.multiple_of(head * size, size)
            move = pltpu.make_async_copy(q_ref.at[:, pl.ds(first, size)], out_ref, sem.at[step])
            move.start()
            moves.append(move)
        for move in moves:
            move.wait()

    return pl.pallas_call(
        kernel,
        in_specs=[SMEM, ANY],
        out_specs=[VMEM] * HEADS,
        out_shape=[pltpu.VMEM((rows, size), jnp.bfloat16)] * HEADS,
        scratch_shapes=[pltpu.SemaphoreType.DMA((HEADS,))],
        compiler_params=params(),
        name="pack_queries",
    )(place, in_hbm(queries))


def unpack_columns(place, back, lane, head_axis):
    rows, size = back[0].shape

    def kernel(place_ref, *refs):
        back_refs, out_ref, sem = refs[:HEADS], refs[HEADS], refs[HEADS + 1]
        moves = []
        for step, ref in enumerate(back_refs):
            head = head_of(place_ref[0] ^ step, lane, head_axis)
            first = pl.multiple_of(head * size, size)
            move = pltpu.make_async_copy(ref, out_ref.at[:, pl.ds(first, size)], sem.at[step])
            move.start()
            moves.append(move)
        for move in moves:
            move.wait()

    return pl.pallas_call(
        kernel,
        in_specs=[SMEM] + [VMEM] * HEADS,
        out_specs=ANY,
        out_shape=pltpu.HBM((rows, HEADS * size), back[0].dtype),
        scratch_shapes=[pltpu.SemaphoreType.DMA((HEADS,))],
        compiler_params=params(),
        name="unpack_columns",
    )(place, *[in_vmem(x) for x in back])


def place_pieces(spot_ref, piece_refs, out_ref, outer, lane, inner):
    if len(piece_refs) == 1:
        out_ref[...] = piece_refs[0][...]
        return
    piece = piece_refs[0].shape[2]
    a, c = spot_ref[0], spot_ref[1]
    spots = [(a, c), (outer - 1 - a, c), (a, inner - 1 - c), (outer - 1 - a, inner - 1 - c)]
    for (at_a, at_c), ref in zip(spots, piece_refs):
        for l in range(lane):
            first = pl.multiple_of(((at_a * lane + l) * inner + at_c) * piece, piece)
            for which in range(3):
                out_ref[which, pl.ds(first, piece), :] = ref[l, which]


def gradients(spot, place, received, pieces, rows, outer, lane, inner, per_run):
    blocks = len(received)
    size = received[0].shape[1]
    runs = blocks // per_run
    half = size // inner
    count = blocks * rows
    group = 2 if blocks % 2 == 0 else 1
    span = group * rows

    def kernel(spot_ref, place_ref, *refs):
        kv_refs, refs = refs[:blocks], refs[blocks:]
        piece_refs, refs = refs[: len(pieces)], refs[len(pieces) :]
        keep_ref, send_ref, tail_ref, last_ref, w_ref = refs[:5]
        kn_ref, hid_ref, tgt_ref, gg_ref, ug_ref, all_ref = refs[5:]
        place_pieces(spot_ref, piece_refs, w_ref, outer, lane, inner)
        for g in range(blocks // group):
            here = slice(g * span, (g + 1) * span)
            mine = range(g * group, (g + 1) * group)

            def stacked(first):
                return jnp.concatenate([kv_refs[b][first : first + rows, :] for b in mine], axis=0)

            key_norm = rms_rows(stacked(0))
            values = stacked(rows).astype(jnp.float32)
            rates = []
            for b in mine:
                row = kv_refs[b][2 * rows : 2 * rows + 1, :rows].astype(jnp.float32)
                rates.append(jnp.broadcast_to(row, (rows, rows)).T)
            rate_columns = jnp.concatenate([jnp.concatenate(rates, axis=0)] * (size // rows), axis=1)
            target = (-rate_columns * values).astype(jnp.bfloat16)
            tgt_ref[here, :] = target
            gate_pre = jnp.dot(key_norm, w_ref[0], preferred_element_type=jnp.float32)
            up_pre = jnp.dot(key_norm, w_ref[1], preferred_element_type=jnp.float32)
            hidden_grad = lax.dot_general(
                target, w_ref[2], (((1,), (1,)), ((), ())), preferred_element_type=jnp.float32
            )
            sigma_gate = jax.nn.sigmoid(gate_pre)
            silu_gate = gate_pre * sigma_gate
            hidden = (silu_gate * up_pre).astype(jnp.bfloat16)
            for part in range(inner):
                columns = slice(part * half, (part + 1) * half)
                kn_ref[part, here, :] = key_norm[:, columns]
                hid_ref[part, here, :] = hidden[:, columns]
            gg_ref[here, :] = (
                hidden_grad * up_pre * sigma_gate * (1.0 + gate_pre * (1.0 - sigma_gate))
            ).astype(jnp.bfloat16)
            ug_ref[here, :] = (hidden_grad * silu_gate).astype(jnp.bfloat16)

        def total(left_ref, right_ref, part):
            return lax.dot_general(
                left_ref[part],
                right_ref[...],
                (((0,), (0,)), ((), ())),
                preferred_element_type=jnp.float32,
            )

        own = spot_ref[1]
        pairs = ((kn_ref, gg_ref), (kn_ref, ug_ref), (hid_ref, tgt_ref))
        for which, (left_ref, right_ref) in enumerate(pairs):
            send_ref[which] = total(left_ref, right_ref, inner - 1 - own).astype(jnp.bfloat16)
            keep_ref[which] = total(left_ref, right_ref, own)
        for step, ref in enumerate(kv_refs):
            block = place_ref[0] ^ step
            for which in range(2):
                end = (which + 1) * rows
                all_ref[block, which * WINDOW : (which + 1) * WINDOW, :] = ref[end - WINDOW : end, :]
        for run in range(runs):
            tail_ref[run] = all_ref[(run + 1) * per_run - 1]
        last_ref[0] = all_ref[blocks - 1]

    return pl.pallas_call(
        kernel,
        in_specs=[SMEM] * 2 + [VMEM] * (blocks + len(pieces)),
        out_specs=[VMEM] * 5,
        out_shape=[
            pltpu.VMEM((3, half, size), jnp.float32),
            pltpu.VMEM((3, half, size), jnp.bfloat16),
            pltpu.VMEM((runs, 2 * WINDOW, size), jnp.bfloat16),
            pltpu.VMEM((1, 2 * WINDOW, size), jnp.bfloat16),
            pltpu.VMEM((3, size, size), jnp.bfloat16),
        ],
        scratch_shapes=[
            pltpu.VMEM((inner, count, half), jnp.bfloat16),
            pltpu.VMEM((inner, count, half), jnp.bfloat16),
            pltpu.VMEM((count, size), jnp.bfloat16),
            pltpu.VMEM((count, size), jnp.bfloat16),
            pltpu.VMEM((count, size), jnp.bfloat16),
            pltpu.VMEM((blocks, 2 * WINDOW, size), jnp.bfloat16),
        ],
        compiler_params=params(20),
        cost_estimate=cost(6),
        name="gradients",
    )(spot, place, *[in_vmem(r) for r in received], *[in_vmem(p) for p in pieces])


def combine(keep, got):
    def kernel(keep_ref, got_ref, out_ref):
        out_ref[...] = (keep_ref[...] + got_ref[...].astype(jnp.float32)).astype(jnp.bfloat16)

    return pl.pallas_call(
        kernel,
        in_specs=[VMEM, VMEM],
        out_specs=VMEM,
        out_shape=pltpu.VMEM(keep.shape, jnp.bfloat16),
        compiler_params=params(),
        name="combine",
    )(in_vmem(keep), in_vmem(got))


def attention(spot, place, queries, received, around, from_outer, old, per_run):
    blocks = len(queries)
    rows, width = queries[0].shape
    span = 2 * WINDOW

    def kernel(spot_ref, place_ref, w_ref, around_ref, outer_ref, *refs):
        q_refs, kv_refs, refs = refs[:blocks], refs[blocks : 2 * blocks], refs[2 * blocks :]
        att_ref, qn_ref, norm_ref, kv_ref, q_ref = refs
        for step in range(blocks):
            kv_ref[place_ref[0] ^ step] = kv_refs[step][: 2 * rows, :]
            q_ref[place_ref[0] ^ step] = q_refs[step][...]
        for which in range(3):
            for first in range(0, width, HEAD_DIM):
                previous = w_ref[which, first : first + HEAD_DIM, :].astype(jnp.float32)
                norm = jnp.sqrt(jnp.mean(previous * previous, axis=1, keepdims=True))
                norm_ref[which, first : first + HEAD_DIM, :] = jnp.broadcast_to(
                    norm, (HEAD_DIM, HEAD_DIM)
                )
        on_first = jnp.where(spot_ref[1] == 0, 1, 0)
        begins = jnp.where(spot_ref[0] == 0, on_first, 0)
        row_id = lax.broadcasted_iota(jnp.int32, (WINDOW, span), 0)
        key_id = lax.broadcasted_iota(jnp.int32, (WINDOW, span), 1)
        allowed = (key_id <= row_id + WINDOW) & (key_id > row_id)
        bias = jnp.where(allowed, 0.0, -1e30)
        first_key = jnp.where(begins == 1, WINDOW, 0)
        first_bias = jnp.where(allowed & (key_id >= first_key), 0.0, -1e30)
        for b in range(blocks):
            qn_ref[b] = rms_rows(q_ref[b])
            pieces = [
                (part, first)
                for part in range(rows // WINDOW)
                for first in range(0, width, HEAD_DIM)
            ]

            def keys_or_values(which, part, first):
                columns = slice(first, first + HEAD_DIM)
                end = which * rows + (part + 1) * WINDOW
                if part:
                    return kv_ref[b, end - span : end, columns]
                before = slice(which * WINDOW, (which + 1) * WINDOW)
                if b % per_run:
                    after = (which + 1) * rows
                    tail = kv_ref[b - 1, after - WINDOW : after, columns]
                elif b:
                    tail = around_ref[b // per_run - on_first, before, columns]
                else:
                    tail = jnp.where(
                        on_first == 1, outer_ref[0, before, columns], around_ref[0, before, columns]
                    )
                return jnp.concatenate([tail, kv_ref[b, end - WINDOW : end, columns]], axis=0)

            masked = []
            for part, first in pieces:
                scores = lax.dot_general(
                    q_ref[b, part * WINDOW : (part + 1) * WINDOW, first : first + HEAD_DIM],
                    keys_or_values(0, part, first),
                    (((1,), (1,)), ((), ())),
                    preferred_element_type=jnp.float32,
                )
                masked.append(
                    scores * (1.0 / math.sqrt(HEAD_DIM)) + (bias if b or part else first_bias)
                )
            masked = jnp.concatenate(masked, axis=0)
            maximum = jnp.max(masked, axis=1, keepdims=True)
            exp_scores = jnp.exp(masked - maximum)
            scale = 1.0 / jnp.sum(exp_scores, axis=1, keepdims=True)
            weights = exp_scores.astype(jnp.bfloat16)
            for i, (part, first) in enumerate(pieces):
                here = slice(i * WINDOW, (i + 1) * WINDOW)
                mixed = jnp.dot(
                    weights[here],
                    keys_or_values(1, part, first),
                    preferred_element_type=jnp.float32,
                )
                att_ref[b, part * WINDOW : (part + 1) * WINDOW, first : first + HEAD_DIM] = (
                    mixed * scale[here]
                )

    return pl.pallas_call(
        kernel,
        in_specs=[SMEM] * 2 + [VMEM] * (3 + 2 * blocks),
        out_specs=[VMEM] * 3,
        out_shape=[
            pltpu.VMEM((blocks, rows, width), jnp.float32),
            pltpu.VMEM((blocks, rows, width), jnp.bfloat16),
            pltpu.VMEM((3, width, HEAD_DIM), jnp.float32),
        ],
        scratch_shapes=[
            pltpu.VMEM((blocks, 2 * rows, width), jnp.bfloat16),
            pltpu.VMEM((blocks, rows, width), jnp.bfloat16),
        ],
        compiler_params=params(10),
        cost_estimate=cost(6),
        name="attention",
    )(
        spot,
        place,
        in_vmem(old),
        in_vmem(around),
        in_vmem(from_outer),
        *[in_vmem(q) for q in queries],
        *[in_vmem(r) for r in received],
    )


def update_and_apply(spot, place, old, norms, sums, query_norm, attended):
    blocks, rows, size = query_norm.shape
    halves = len(sums) // 2
    half = size // halves
    group = 2 if blocks % 2 == 0 else 1

    def kernel(spot_ref, place_ref, w_ref, norm_ref, *refs):
        sum_refs, refs = refs[: 2 * halves], refs[2 * halves :]
        q_ref, a_ref, out_refs, (total_ref, new_ref) = refs[0], refs[1], refs[2:-2], refs[-2:]
        squares = jnp.zeros((8, size), jnp.float32)
        for part in range(halves):
            place = spot_ref[1] if part == 0 else halves - 1 - spot_ref[1]
            for which in range(3):
                total = sum_refs[2 * part][which].astype(jnp.float32) + sum_refs[2 * part + 1][
                    which
                ].astype(jnp.float32)
                total_ref[place, which] = total
                squares = squares + jnp.sum(
                    (total * total).reshape(half // 8, 8, size), axis=0
                )
        norm_scale = lax.rsqrt(
            jnp.sum(squares, axis=(0, 1), keepdims=True) / (3 * size * size) + NORM_EPS
        )
        scale = STEP_SIZE * norm_scale
        for part in range(halves):
            for which in range(3):
                here = slice(part * half, (part + 1) * half)
                previous = w_ref[which, here, :].astype(jnp.float32)
                stepped = previous - scale * total_ref[part, which]
                factor = norm_ref[which, here, 0:1] * lax.rsqrt(
                    jnp.mean(stepped * stepped, axis=1, keepdims=True) + NORM_EPS
                )
                new_ref[which, here, :] = (stepped * factor).astype(jnp.bfloat16)
        for g in range(blocks // group):
            steps = range(g * group, (g + 1) * group)
            mine = [place_ref[0] ^ step for step in steps]
            query = jnp.concatenate([q_ref[b] for b in mine], axis=0)
            query_gate = jnp.dot(query, new_ref[0], preferred_element_type=jnp.float32)
            query_up = jnp.dot(query, new_ref[1], preferred_element_type=jnp.float32)
            query_hidden = (query_gate * jax.nn.sigmoid(query_gate) * query_up).astype(
                jnp.bfloat16
            )
            fast = jnp.dot(query_hidden, new_ref[2], preferred_element_type=jnp.float32).astype(
                jnp.bfloat16
            )
            for i, (step, b) in enumerate(zip(steps, mine)):
                out_refs[step][...] = (
                    a_ref[b] + fast[i * rows : (i + 1) * rows, :].astype(jnp.float32)
                ).astype(jnp.bfloat16)

    return pl.pallas_call(
        kernel,
        in_specs=[SMEM] * 2 + [VMEM] * (len(sums) + 4),
        out_specs=[VMEM] * blocks,
        out_shape=[pltpu.VMEM((rows, size), jnp.bfloat16)] * blocks,
        scratch_shapes=[
            pltpu.VMEM((halves, 3, half, size), jnp.float32),
            pltpu.VMEM((3, size, size), jnp.bfloat16),
        ],
        compiler_params=params(16),
        cost_estimate=cost(6),
        name="update_and_apply",
    )(
        spot,
        place,
        in_vmem(old),
        in_vmem(norms),
        *[in_vmem(s) for s in sums],
        in_vmem(query_norm),
        in_vmem(attended),
    )


def gather_rows(mine, axis, count, index, order_axis):
    if count & (count - 1):
        return lax.all_gather(mine, axis, axis=order_axis, tiled=True)
    stride = 1
    while stride < count:
        theirs = lax.ppermute(mine, axis, swap_pairs(count, stride))
        low = (index // stride) % 2 == 0
        mine = jnp.concatenate(
            [jnp.where(low, mine, theirs), jnp.where(low, theirs, mine)], order_axis
        )
        stride *= 2
    return mine


def make_shards(outer, lane, inner, head_axis):
    group = ("lane", "head")

    def shards(queries, key_rows, value_rows, step_rates, w_gate, w_up, w_down):
        rows, width = queries.shape
        size = width // HEADS
        a = lax.axis_index("outer")
        c = lax.axis_index("inner")
        spot = jnp.stack([a, c]).astype(jnp.int32)
        place = jnp.reshape(lax.axis_index(group), (1,)).astype(jnp.int32)
        spot, place, w_gate = lax.optimization_barrier((spot, place, w_gate))

        own, *packed = pack(
            place,
            key_rows,
            value_rows,
            jnp.transpose(step_rates),
            w_gate,
            w_up,
            w_down,
            lane,
            head_axis,
        )
        if lane > 1:
            own = lax.all_to_all(own, "lane", split_axis=0, concat_axis=0, tiled=True)

        def exchange(chunks):
            got = [chunks[0]]
            for step in range(1, HEADS):
                got.append(lax.ppermute(chunks[step], group, swap_pairs(HEADS, step)))
            return got

        kv = exchange(packed)
        qs = pack_queries(place, queries, lane, head_axis)
        qs = exchange(qs)

        if outer == 2 and inner == 2:
            other = lax.ppermute(own, "outer", swap_pairs(outer, 1))
            own_beside = lax.ppermute(own, "inner", swap_pairs(inner, 1))
            other_beside = lax.ppermute(other, "inner", swap_pairs(inner, 1))
            pieces = [own, other, own_beside, other_beside]
        else:
            old = gather_rows(own[None], "outer", outer, a, 0)[:, :, None]
            old = gather_rows(old, "inner", inner, c, 2)
            pieces = [jnp.transpose(old, (3, 0, 1, 2, 4, 5)).reshape(3, size, size)]

        keep, send, tails, last, old = gradients(
            spot, place, kv, pieces, rows, outer, lane, inner, head_axis
        )
        if inner > 1:
            got = lax.ppermute(send, "inner", swap_pairs(inner, 1))
            half = combine(keep, got)
        else:
            half = keep.astype(jnp.bfloat16)
        mine, theirs = half, jnp.zeros_like(half)
        if outer & (outer - 1):
            mine = lax.psum(half, "outer")
        else:
            stride = 1
            while stride < outer:
                if stride > 1:
                    mine = (mine.astype(jnp.float32) + theirs.astype(jnp.float32)).astype(
                        jnp.bfloat16
                    )
                theirs = lax.ppermute(mine, "outer", swap_pairs(outer, stride))
                stride *= 2
        around = tails
        if inner > 1:
            around = lax.ppermute(tails, "inner", [(i, (i + 1) % inner) for i in range(inner)])
        pairs = [
            (i * inner + inner - 1, (i + 1) * inner) for i in range(outer - 1)
        ]
        from_outer = lax.ppermute(last, ("outer", "inner"), pairs) if pairs else last
        attended, query_norm, norms = attention(
            spot, place, qs, kv, around, from_outer, old, head_axis
        )

        theirs, attended, query_norm, norms = lax.optimization_barrier(
            (theirs, attended, query_norm, norms)
        )
        sums = [mine, theirs]
        if inner > 1:
            sums.append(lax.ppermute(mine, "inner", swap_pairs(inner, 1)))
            sums.append(lax.ppermute(theirs, "inner", swap_pairs(inner, 1)))

        out = update_and_apply(spot, place, old, norms, sums, query_norm, attended)
        return unpack_columns(place, exchange(out), lane, head_axis)

    return shards


def solution(mesh):
    seq, head_axis = mesh.shape["seq"], mesh.shape["head"]
    lane = HEADS // head_axis
    inner = 2 if (seq // lane) % 2 == 0 else 1
    outer = seq // lane // inner
    names = ("outer", "lane", "inner", "head")
    split = Mesh(mesh.devices.reshape(outer, lane, inner, head_axis), names)
    rows = P(names, None)
    weights = P(names[:3], names[3], None)
    shards = make_shards(outer, lane, inner, head_axis)

    return jax.shard_map(
        shards,
        mesh=split,
        in_specs=(rows, rows, rows, rows, weights, weights, weights),
        out_specs=rows,
        check_vma=False,
    )
```

```python
import math

import jax
import jax.numpy as jnp
from jax import lax
from jax.experimental import pallas as pl
from jax.experimental.pallas import tpu as pltpu
from jax.sharding import Mesh, PartitionSpec as P


HEADS = 8
HEAD_DIM = 128
WINDOW = 64
STEP_SIZE = 0.05
NORM_EPS = 1e-06
RATE_ROWS = 8
ANY = pl.BlockSpec(memory_space=pl.ANY)
VMEM = pl.BlockSpec(memory_space=pltpu.VMEM)
SMEM = pl.BlockSpec(memory_space=pltpu.SMEM)


def in_vmem(x):
    return pltpu.with_memory_space_constraint(x, pltpu.VMEM)


def in_hbm(x):
    return pltpu.with_memory_space_constraint(x, pltpu.HBM)


def cost(microseconds):
    return pl.CostEstimate(
        flops=int(microseconds * 4e6), bytes_accessed=1 << 20, transcendentals=0
    )


def params(mib=4):
    return pltpu.CompilerParams(vmem_limit_bytes=mib << 20)


def swap_pairs(count, stride):
    return [(i, i ^ stride) for i in range(count)]


def rms_rows(rows):
    wide = rows.astype(jnp.float32)
    scale = lax.rsqrt(jnp.mean(wide * wide, axis=1, keepdims=True) + NORM_EPS)
    return (wide * scale).astype(jnp.bfloat16)


def head_of(peer, lane, head_axis):
    return (peer % head_axis) * lane + peer // head_axis


def pack(place, key_rows, value_rows, rates_t, w_gate, w_up, w_down, lane, head_axis):
    rows, width = key_rows.shape
    size = width // HEADS
    piece, local, _ = w_gate.shape

    def kernel(place_ref, k_ref, v_ref, r_ref, g_ref, u_ref, d_ref, w_out_ref, *refs):
        out_refs, w_refs, (sem, w_sem) = refs[:HEADS], refs[HEADS : HEADS + 3], refs[HEADS + 3 :]
        loads = [
            pltpu.make_async_copy(src, dst, w_sem.at[i])
            for i, (src, dst) in enumerate(zip((g_ref, u_ref, d_ref), w_refs))
        ]
        for load in loads:
            load.start()
        moves = []
        heads = []
        for step, out_ref in enumerate(out_refs):
            head = head_of(place_ref[0] ^ step, lane, head_axis)
            heads.append(head)
            first = pl.multiple_of(head * size, size)
            for which, ref in enumerate((k_ref, v_ref)):
                move = pltpu.make_async_copy(
                    ref.at[:, pl.ds(first, size)],
                    out_ref.at[pl.ds(which * rows, rows), :],
                    sem.at[len(moves)],
                )
                move.start()
                moves.append(move)
        rates = r_ref[...].astype(jnp.float32)
        head_id = lax.broadcasted_iota(jnp.int32, rates.shape, 0)
        for head, out_ref in zip(heads, out_refs):
            row = jnp.sum(jnp.where(head_id == head, rates, 0.0), axis=0, keepdims=True)
            wide = jnp.broadcast_to(row, (RATE_ROWS, rows)).astype(jnp.bfloat16)
            for first in range(0, size, rows):
                out_ref[2 * rows :, first : first + rows] = wide
        for which, (load, ref) in enumerate(zip(loads, w_refs)):
            load.wait()
            for head in range(local):
                w_out_ref[head, which] = ref[:, head, :]
        for move in moves:
            move.wait()

    return pl.pallas_call(
        kernel,
        in_specs=[SMEM, ANY, ANY, VMEM, ANY, ANY, ANY],
        out_specs=[VMEM] * (1 + HEADS),
        out_shape=[pltpu.HBM((local, 3, piece, size), jnp.bfloat16)]
        + [pltpu.VMEM((2 * rows + RATE_ROWS, size), jnp.bfloat16)] * HEADS,
        scratch_shapes=[pltpu.VMEM(w_gate.shape, w_gate.dtype)] * 3
        + [pltpu.SemaphoreType.DMA((HEADS * 2,)), pltpu.SemaphoreType.DMA((3,))],
        compiler_params=params(),
        name="pack",
    )(place, *[in_hbm(x) for x in (key_rows, value_rows, rates_t, w_gate, w_up, w_down)])


def pack_queries(place, queries, lane, head_axis):
    rows, width = queries.shape
    size = width // HEADS

    def kernel(place_ref, q_ref, *refs):
        out_refs, sem = refs[:HEADS], refs[HEADS]
        moves = []
        for step, out_ref in enumerate(out_refs):
            head = head_of(place_ref[0] ^ step, lane, head_axis)
            first = pl.multiple_of(head * size, size)
            move = pltpu.make_async_copy(q_ref.at[:, pl.ds(first, size)], out_ref, sem.at[step])
            move.start()
            moves.append(move)
        for move in moves:
            move.wait()

    return pl.pallas_call(
        kernel,
        in_specs=[SMEM, ANY],
        out_specs=[VMEM] * HEADS,
        out_shape=[pltpu.VMEM((rows, size), jnp.bfloat16)] * HEADS,
        scratch_shapes=[pltpu.SemaphoreType.DMA((HEADS,))],
        compiler_params=params(),
        name="pack_queries",
    )(place, in_hbm(queries))


def unpack_columns(place, back, lane, head_axis):
    rows, size = back[0].shape

    def kernel(place_ref, *refs):
        back_refs, out_ref, sem = refs[:HEADS], refs[HEADS], refs[HEADS + 1]
        moves = []
        for step, ref in enumerate(back_refs):
            head = head_of(place_ref[0] ^ step, lane, head_axis)
            first = pl.multiple_of(head * size, size)
            move = pltpu.make_async_copy(ref, out_ref.at[:, pl.ds(first, size)], sem.at[step])
            move.start()
            moves.append(move)
        for move in moves:
            move.wait()

    return pl.pallas_call(
        kernel,
        in_specs=[SMEM] + [VMEM] * HEADS,
        out_specs=ANY,
        out_shape=pltpu.HBM((rows, HEADS * size), back[0].dtype),
        scratch_shapes=[pltpu.SemaphoreType.DMA((HEADS,))],
        compiler_params=params(),
        name="unpack_columns",
    )(place, *[in_vmem(x) for x in back])


def place_pieces(spot_ref, piece_refs, out_ref, outer, lane, inner):
    if len(piece_refs) == 1:
        out_ref[...] = piece_refs[0][...]
        return
    piece = piece_refs[0].shape[2]
    a, c = spot_ref[0], spot_ref[1]
    spots = [(a, c), (outer - 1 - a, c), (a, inner - 1 - c), (outer - 1 - a, inner - 1 - c)]
    for (at_a, at_c), ref in zip(spots, piece_refs):
        for l in range(lane):
            first = pl.multiple_of(((at_a * lane + l) * inner + at_c) * piece, piece)
            for which in range(ref.shape[1]):
                out_ref[which, pl.ds(first, piece), :] = ref[l, which]


def split_pieces(own):
    lane, _, piece, size = own.shape

    def kernel(own_ref, first_ref, last_ref):
        for l in range(lane):
            first_ref[l] = own_ref[l, :2]
            last_ref[l] = own_ref[l, 2:]

    return pl.pallas_call(
        kernel,
        in_specs=[VMEM],
        out_specs=[VMEM] * 2,
        out_shape=[
            pltpu.VMEM((lane, 2, piece, size), own.dtype),
            pltpu.VMEM((lane, 1, piece, size), own.dtype),
        ],
        compiler_params=params(),
        name="split_pieces",
    )(in_vmem(own))


def total_of(left_ref, right_ref, part):
    return lax.dot_general(
        left_ref[part], right_ref[...], (((0,), (0,)), ((), ())), preferred_element_type=jnp.float32
    )


def down_gradient(spot, place, received, pieces, rows, outer, lane, inner, per_run):
    blocks = len(received)
    size = received[0].shape[1]
    runs = blocks // per_run
    half = size // inner
    count = blocks * rows
    group = 2 if blocks % 2 == 0 else 1
    span = group * rows

    def kernel(spot_ref, place_ref, *refs):
        kv_refs, refs = refs[:blocks], refs[blocks:]
        piece_refs, refs = refs[: len(pieces)], refs[len(pieces) :]
        keep_ref, send_ref, tail_ref, last_ref, w_ref, kn_ref, tgt_ref, gf_ref, uf_ref = refs[:9]
        hid_ref, all_ref = refs[9:]
        place_pieces(spot_ref, piece_refs, w_ref, outer, lane, inner)
        for g in range(blocks // group):
            here = slice(g * span, (g + 1) * span)
            mine = range(g * group, (g + 1) * group)

            def stacked(first):
                return jnp.concatenate([kv_refs[b][first : first + rows, :] for b in mine], axis=0)

            key_norm = rms_rows(stacked(0))
            values = stacked(rows).astype(jnp.float32)
            rates = []
            for b in mine:
                row = kv_refs[b][2 * rows : 2 * rows + 1, :rows].astype(jnp.float32)
                rates.append(jnp.broadcast_to(row, (rows, rows)).T)
            rate_columns = jnp.concatenate([jnp.concatenate(rates, axis=0)] * (size // rows), axis=1)
            tgt_ref[here, :] = (-rate_columns * values).astype(jnp.bfloat16)
            gate_pre = jnp.dot(key_norm, w_ref[0], preferred_element_type=jnp.float32)
            up_pre = jnp.dot(key_norm, w_ref[1], preferred_element_type=jnp.float32)
            sigma_gate = jax.nn.sigmoid(gate_pre)
            silu_gate = gate_pre * sigma_gate
            hidden = (silu_gate * up_pre).astype(jnp.bfloat16)
            for part in range(inner):
                columns = slice(part * half, (part + 1) * half)
                kn_ref[part, here, :] = key_norm[:, columns]
                hid_ref[part, here, :] = hidden[:, columns]
            gf_ref[here, :] = up_pre * sigma_gate * (1.0 + gate_pre * (1.0 - sigma_gate))
            uf_ref[here, :] = silu_gate
        own = spot_ref[1]
        send_ref[0] = total_of(hid_ref, tgt_ref, inner - 1 - own).astype(jnp.bfloat16)
        keep_ref[0] = total_of(hid_ref, tgt_ref, own)
        for step, ref in enumerate(kv_refs):
            block = place_ref[0] ^ step
            for which in range(2):
                end = (which + 1) * rows
                all_ref[block, which * WINDOW : (which + 1) * WINDOW, :] = ref[end - WINDOW : end, :]
        for run in range(runs):
            tail_ref[run] = all_ref[(run + 1) * per_run - 1]
        last_ref[0] = all_ref[blocks - 1]

    return pl.pallas_call(
        kernel,
        in_specs=[SMEM] * 2 + [VMEM] * (blocks + len(pieces)),
        out_specs=[VMEM] * 9,
        out_shape=[
            pltpu.VMEM((1, half, size), jnp.float32),
            pltpu.VMEM((1, half, size), jnp.bfloat16),
            pltpu.VMEM((runs, 2 * WINDOW, size), jnp.bfloat16),
            pltpu.VMEM((1, 2 * WINDOW, size), jnp.bfloat16),
            pltpu.VMEM((2, size, size), jnp.bfloat16),
            pltpu.VMEM((inner, count, half), jnp.bfloat16),
            pltpu.VMEM((count, size), jnp.bfloat16),
            pltpu.VMEM((count, size), jnp.float32),
            pltpu.VMEM((count, size), jnp.float32),
        ],
        scratch_shapes=[
            pltpu.VMEM((inner, count, half), jnp.bfloat16),
            pltpu.VMEM((blocks, 2 * WINDOW, size), jnp.bfloat16),
        ],
        compiler_params=params(14),
        cost_estimate=cost(4),
        name="down_gradient",
    )(spot, place, *[in_vmem(r) for r in received], *[in_vmem(p) for p in pieces])


def other_gradients(spot, pieces, key_norm, target, gate_factor, up_factor, outer, lane):
    inner, count, half = key_norm.shape
    size = target.shape[1]
    span = count // 4

    def kernel(spot_ref, *refs):
        piece_refs, refs = refs[: len(pieces)], refs[len(pieces) :]
        kn_ref, tgt_ref, gf_ref, uf_ref, keep_ref, send_ref, w_ref, gg_ref, ug_ref = refs
        place_pieces(spot_ref, piece_refs, w_ref, outer, lane, inner)
        for first in range(0, count, span):
            here = slice(first, first + span)
            hidden_grad = lax.dot_general(
                tgt_ref[here, :],
                w_ref[0],
                (((1,), (1,)), ((), ())),
                preferred_element_type=jnp.float32,
            )
            gg_ref[here, :] = (hidden_grad * gf_ref[here, :]).astype(jnp.bfloat16)
            ug_ref[here, :] = (hidden_grad * uf_ref[here, :]).astype(jnp.bfloat16)
        own = spot_ref[1]
        for which, right_ref in enumerate((gg_ref, ug_ref)):
            send_ref[which] = total_of(kn_ref, right_ref, inner - 1 - own).astype(jnp.bfloat16)
            keep_ref[which] = total_of(kn_ref, right_ref, own)

    return pl.pallas_call(
        kernel,
        in_specs=[SMEM] + [VMEM] * (len(pieces) + 4),
        out_specs=[VMEM] * 3,
        out_shape=[
            pltpu.VMEM((2, half, size), jnp.float32),
            pltpu.VMEM((2, half, size), jnp.bfloat16),
            pltpu.VMEM((1, size, size), jnp.bfloat16),
        ],
        scratch_shapes=[pltpu.VMEM((count, size), jnp.bfloat16)] * 2,
        compiler_params=params(10),
        cost_estimate=cost(3),
        name="other_gradients",
    )(
        spot,
        *[in_vmem(p) for p in pieces],
        *[in_vmem(x) for x in (key_norm, target, gate_factor, up_factor)],
    )


def combine(keep, got):
    def kernel(keep_ref, got_ref, out_ref):
        out_ref[...] = (keep_ref[...] + got_ref[...].astype(jnp.float32)).astype(jnp.bfloat16)

    return pl.pallas_call(
        kernel,
        in_specs=[VMEM, VMEM],
        out_specs=VMEM,
        out_shape=pltpu.VMEM(keep.shape, jnp.bfloat16),
        compiler_params=params(),
        name="combine",
    )(in_vmem(keep), in_vmem(got))


def attention(spot, place, queries, received, around, from_outer, old_first, old_last, per_run):
    blocks = len(queries)
    rows, width = queries[0].shape
    span = 2 * WINDOW

    def kernel(spot_ref, place_ref, w_ref, w_last_ref, around_ref, outer_ref, *refs):
        q_refs, kv_refs, refs = refs[:blocks], refs[blocks : 2 * blocks], refs[2 * blocks :]
        att_ref, qn_ref, norm_ref, kv_ref, q_ref = refs
        for step in range(blocks):
            kv_ref[place_ref[0] ^ step] = kv_refs[step][: 2 * rows, :]
            q_ref[place_ref[0] ^ step] = q_refs[step][...]
        for which in range(3):
            for first in range(0, width, HEAD_DIM):
                source, index = (w_ref, which) if which < 2 else (w_last_ref, 0)
                previous = source[index, first : first + HEAD_DIM, :].astype(jnp.float32)
                norm = jnp.sqrt(jnp.mean(previous * previous, axis=1, keepdims=True))
                norm_ref[which, first : first + HEAD_DIM, :] = jnp.broadcast_to(
                    norm, (HEAD_DIM, HEAD_DIM)
                )
        on_first = jnp.where(spot_ref[1] == 0, 1, 0)
        begins = jnp.where(spot_ref[0] == 0, on_first, 0)
        row_id = lax.broadcasted_iota(jnp.int32, (WINDOW, span), 0)
        key_id = lax.broadcasted_iota(jnp.int32, (WINDOW, span), 1)
        allowed = (key_id <= row_id + WINDOW) & (key_id > row_id)
        bias = jnp.where(allowed, 0.0, -1e30)
        first_key = jnp.where(begins == 1, WINDOW, 0)
        first_bias = jnp.where(allowed & (key_id >= first_key), 0.0, -1e30)
        for b in range(blocks):
            qn_ref[b] = rms_rows(q_ref[b])
            pieces = [
                (part, first)
                for part in range(rows // WINDOW)
                for first in range(0, width, HEAD_DIM)
            ]

            def keys_or_values(which, part, first):
                columns = slice(first, first + HEAD_DIM)
                end = which * rows + (part + 1) * WINDOW
                if part:
                    return kv_ref[b, end - span : end, columns]
                before = slice(which * WINDOW, (which + 1) * WINDOW)
                if b % per_run:
                    after = (which + 1) * rows
                    tail = kv_ref[b - 1, after - WINDOW : after, columns]
                elif b:
                    tail = around_ref[b // per_run - on_first, before, columns]
                else:
                    tail = jnp.where(
                        on_first == 1, outer_ref[0, before, columns], around_ref[0, before, columns]
                    )
                return jnp.concatenate([tail, kv_ref[b, end - WINDOW : end, columns]], axis=0)

            masked = []
            for part, first in pieces:
                scores = lax.dot_general(
                    q_ref[b, part * WINDOW : (part + 1) * WINDOW, first : first + HEAD_DIM],
                    keys_or_values(0, part, first),
                    (((1,), (1,)), ((), ())),
                    preferred_element_type=jnp.float32,
                )
                masked.append(
                    scores * (1.0 / math.sqrt(HEAD_DIM)) + (bias if b or part else first_bias)
                )
            masked = jnp.concatenate(masked, axis=0)
            maximum = jnp.max(masked, axis=1, keepdims=True)
            exp_scores = jnp.exp(masked - maximum)
            scale = 1.0 / jnp.sum(exp_scores, axis=1, keepdims=True)
            weights = exp_scores.astype(jnp.bfloat16)
            for i, (part, first) in enumerate(pieces):
                here = slice(i * WINDOW, (i + 1) * WINDOW)
                mixed = jnp.dot(
                    weights[here],
                    keys_or_values(1, part, first),
                    preferred_element_type=jnp.float32,
                )
                att_ref[b, part * WINDOW : (part + 1) * WINDOW, first : first + HEAD_DIM] = (
                    mixed * scale[here]
                )

    return pl.pallas_call(
        kernel,
        in_specs=[SMEM] * 2 + [VMEM] * (4 + 2 * blocks),
        out_specs=[VMEM] * 3,
        out_shape=[
            pltpu.VMEM((blocks, rows, width), jnp.float32),
            pltpu.VMEM((blocks, rows, width), jnp.bfloat16),
            pltpu.VMEM((3, width, HEAD_DIM), jnp.float32),
        ],
        scratch_shapes=[
            pltpu.VMEM((blocks, 2 * rows, width), jnp.bfloat16),
            pltpu.VMEM((blocks, rows, width), jnp.bfloat16),
        ],
        compiler_params=params(10),
        cost_estimate=cost(6),
        name="attention",
    )(
        spot,
        place,
        in_vmem(old_first),
        in_vmem(old_last),
        in_vmem(around),
        in_vmem(from_outer),
        *[in_vmem(q) for q in queries],
        *[in_vmem(r) for r in received],
    )


def update_and_apply(spot, place, old_first, old_last, norms, first, last, query_norm, attended):
    sums = first + last
    blocks, rows, size = query_norm.shape
    halves = len(first) // 2
    half = size // halves
    group = 2 if blocks % 2 == 0 else 1

    def kernel(spot_ref, place_ref, w_ref, w_last_ref, norm_ref, *refs):
        sum_refs, refs = refs[: len(sums)], refs[len(sums) :]
        q_ref, a_ref, out_refs, (total_ref, new_ref) = refs[0], refs[1], refs[2:-2], refs[-2:]
        squares = jnp.zeros((8, size), jnp.float32)
        for part in range(halves):
            place = spot_ref[1] if part == 0 else halves - 1 - spot_ref[1]
            for which in range(3):
                begin, index = (2 * part, which) if which < 2 else (2 * halves + 2 * part, 0)
                total = sum_refs[begin][index].astype(jnp.float32) + sum_refs[begin + 1][
                    index
                ].astype(jnp.float32)
                total_ref[place, which] = total
                squares = squares + jnp.sum(
                    (total * total).reshape(half // 8, 8, size), axis=0
                )
        norm_scale = lax.rsqrt(
            jnp.sum(squares, axis=(0, 1), keepdims=True) / (3 * size * size) + NORM_EPS
        )
        scale = STEP_SIZE * norm_scale
        for part in range(halves):
            for which in range(3):
                here = slice(part * half, (part + 1) * half)
                source, index = (w_ref, which) if which < 2 else (w_last_ref, 0)
                previous = source[index, here, :].astype(jnp.float32)
                stepped = previous - scale * total_ref[part, which]
                factor = norm_ref[which, here, 0:1] * lax.rsqrt(
                    jnp.mean(stepped * stepped, axis=1, keepdims=True) + NORM_EPS
                )
                new_ref[which, here, :] = (stepped * factor).astype(jnp.bfloat16)
        for g in range(blocks // group):
            steps = range(g * group, (g + 1) * group)
            mine = [place_ref[0] ^ step for step in steps]
            query = jnp.concatenate([q_ref[b] for b in mine], axis=0)
            query_gate = jnp.dot(query, new_ref[0], preferred_element_type=jnp.float32)
            query_up = jnp.dot(query, new_ref[1], preferred_element_type=jnp.float32)
            query_hidden = (query_gate * jax.nn.sigmoid(query_gate) * query_up).astype(
                jnp.bfloat16
            )
            fast = jnp.dot(query_hidden, new_ref[2], preferred_element_type=jnp.float32).astype(
                jnp.bfloat16
            )
            for i, (step, b) in enumerate(zip(steps, mine)):
                out_refs[step][...] = (
                    a_ref[b] + fast[i * rows : (i + 1) * rows, :].astype(jnp.float32)
                ).astype(jnp.bfloat16)

    return pl.pallas_call(
        kernel,
        in_specs=[SMEM] * 2 + [VMEM] * (len(sums) + 5),
        out_specs=[VMEM] * blocks,
        out_shape=[pltpu.VMEM((rows, size), jnp.bfloat16)] * blocks,
        scratch_shapes=[
            pltpu.VMEM((halves, 3, half, size), jnp.float32),
            pltpu.VMEM((3, size, size), jnp.bfloat16),
        ],
        compiler_params=params(16),
        cost_estimate=cost(6),
        name="update_and_apply",
    )(
        spot,
        place,
        in_vmem(old_first),
        in_vmem(old_last),
        in_vmem(norms),
        *[in_vmem(s) for s in sums],
        in_vmem(query_norm),
        in_vmem(attended),
    )


def gather_rows(mine, axis, count, index, order_axis):
    if count & (count - 1):
        return lax.all_gather(mine, axis, axis=order_axis, tiled=True)
    stride = 1
    while stride < count:
        theirs = lax.ppermute(mine, axis, swap_pairs(count, stride))
        low = (index // stride) % 2 == 0
        mine = jnp.concatenate(
            [jnp.where(low, mine, theirs), jnp.where(low, theirs, mine)], order_axis
        )
        stride *= 2
    return mine


def make_shards(outer, lane, inner, head_axis):
    group = ("lane", "head")

    def shards(queries, key_rows, value_rows, step_rates, w_gate, w_up, w_down):
        rows, width = queries.shape
        size = width // HEADS
        a = lax.axis_index("outer")
        c = lax.axis_index("inner")
        spot = jnp.stack([a, c]).astype(jnp.int32)
        place = jnp.reshape(lax.axis_index(group), (1,)).astype(jnp.int32)
        spot, place, w_gate = lax.optimization_barrier((spot, place, w_gate))

        own, *packed = pack(
            place,
            key_rows,
            value_rows,
            jnp.transpose(step_rates),
            w_gate,
            w_up,
            w_down,
            lane,
            head_axis,
        )
        if lane > 1:
            own = lax.all_to_all(own, "lane", split_axis=0, concat_axis=0, tiled=True)

        def exchange(chunks):
            got = [chunks[0]]
            for step in range(1, HEADS):
                got.append(lax.ppermute(chunks[step], group, swap_pairs(HEADS, step)))
            return got

        kv = exchange(packed)
        qs = pack_queries(place, queries, lane, head_axis)
        qs = exchange(qs)

        if outer == 2 and inner == 2:
            first_pieces, last_pieces = ([part] for part in split_pieces(own))
            for pieces in (first_pieces, last_pieces):
                pieces.append(lax.ppermute(pieces[0], "outer", swap_pairs(outer, 1)))
                pieces.append(lax.ppermute(pieces[0], "inner", swap_pairs(inner, 1)))
                pieces.append(lax.ppermute(pieces[1], "inner", swap_pairs(inner, 1)))
        else:
            old = gather_rows(own[None], "outer", outer, a, 0)[:, :, None]
            old = gather_rows(old, "inner", inner, c, 2)
            old = jnp.transpose(old, (3, 0, 1, 2, 4, 5)).reshape(3, size, size)
            first_pieces, last_pieces = [old[:2]], [old[2:]]

        def begin_sum(keep, send):
            half = keep.astype(jnp.bfloat16)
            if inner > 1:
                got = lax.ppermute(send, "inner", swap_pairs(inner, 1))
                half = combine(keep, got)
            mine, theirs = half, jnp.zeros_like(half)
            if outer & (outer - 1):
                return lax.psum(half, "outer"), theirs
            stride = 1
            while stride < outer:
                if stride > 1:
                    mine = (mine.astype(jnp.float32) + theirs.astype(jnp.float32)).astype(
                        jnp.bfloat16
                    )
                theirs = lax.ppermute(mine, "outer", swap_pairs(outer, stride))
                stride *= 2
            return mine, theirs

        def share(value):
            return lax.ppermute(value, "inner", swap_pairs(inner, 1))

        keep, send, tails, last, old_first, *rest = down_gradient(
            spot, place, kv, first_pieces, rows, outer, lane, inner, head_axis
        )
        last_sums = list(begin_sum(keep, send))
        keep, send, old_last = other_gradients(spot, last_pieces, *rest, outer, lane)
        first_sums = list(begin_sum(keep, send))
        around = tails
        if inner > 1:
            around = lax.ppermute(tails, "inner", [(i, (i + 1) % inner) for i in range(inner)])
        pairs = [
            (i * inner + inner - 1, (i + 1) * inner) for i in range(outer - 1)
        ]
        from_outer = lax.ppermute(last, ("outer", "inner"), pairs) if pairs else last
        attended, query_norm, norms = attention(spot, place, qs, kv, around, from_outer, old_first, old_last, head_axis)

        first_sums[1], attended, query_norm, norms = lax.optimization_barrier(
            (first_sums[1], attended, query_norm, norms)
        )
        if inner > 1:
            last_sums += [share(last_sums[0]), share(last_sums[1])]
            first_sums += [share(first_sums[0]), share(first_sums[1])]

        out = update_and_apply(
            spot, place, old_first, old_last, norms, first_sums, last_sums, query_norm, attended
        )
        return unpack_columns(place, exchange(out), lane, head_axis)

    return shards


def solution(mesh):
    seq, head_axis = mesh.shape["seq"], mesh.shape["head"]
    lane = HEADS // head_axis
    inner = 2 if (seq // lane) % 2 == 0 else 1
    outer = seq // lane // inner
    names = ("outer", "lane", "inner", "head")
    split = Mesh(mesh.devices.reshape(outer, lane, inner, head_axis), names)
    rows = P(names, None)
    weights = P(names[:3], names[3], None)
    shards = make_shards(outer, lane, inner, head_axis)

    return jax.shard_map(
        shards,
        mesh=split,
        in_specs=(rows, rows, rows, rows, weights, weights, weights),
        out_specs=rows,
        check_vma=False,
    )
```

```python
import math

import jax
import jax.numpy as jnp
from jax import lax
from jax.experimental import pallas as pl
from jax.experimental.pallas import tpu as pltpu
from jax.sharding import Mesh, PartitionSpec as P


HEADS = 8
HEAD_DIM = 128
WINDOW = 64
STEP_SIZE = 0.05
NORM_EPS = 1e-06
RATE_ROWS = 8
STRIP = 32
KEY_STEPS = (4, 7, 6, 5, 3, 2, 1)
ANY = pl.BlockSpec(memory_space=pl.ANY)
VMEM = pl.BlockSpec(memory_space=pltpu.VMEM)
SMEM = pl.BlockSpec(memory_space=pltpu.SMEM)


def in_vmem(x):
    return pltpu.with_memory_space_constraint(x, pltpu.VMEM)


def in_hbm(x):
    return pltpu.with_memory_space_constraint(x, pltpu.HBM)


def cost(microseconds):
    return pl.CostEstimate(
        flops=int(microseconds * 4e6), bytes_accessed=1 << 20, transcendentals=0
    )


def params(mib=4):
    return pltpu.CompilerParams(vmem_limit_bytes=mib << 20)


def swap_pairs(count, stride):
    return [(i, i ^ stride) for i in range(count)]


def rms_rows(rows):
    wide = rows.astype(jnp.float32)
    scale = lax.rsqrt(jnp.mean(wide * wide, axis=1, keepdims=True) + NORM_EPS)
    return (wide * scale).astype(jnp.bfloat16)


def head_of(peer, lane, head_axis):
    return (peer % head_axis) * lane + peer // head_axis


def pack(place, key_rows, value_rows, rates_t, steps, weights, lane, head_axis):
    rows, width = key_rows.shape
    size = width // HEADS
    count, loaded = len(steps), len(weights)

    def kernel(place_ref, k_ref, v_ref, r_ref, *refs):
        given_refs, refs = refs[:loaded], refs[loaded:]
        out_refs, refs = refs[:count], refs[count:]
        moves = []
        heads = []
        if loaded:
            w_out_ref, w_refs, w_sem = refs[0], refs[2:-1], refs[-1]
            sem = refs[1]
            loads = [
                pltpu.make_async_copy(src, dst, w_sem.at[i])
                for i, (src, dst) in enumerate(zip(given_refs, w_refs))
            ]
            for load in loads:
                load.start()
        else:
            sem = refs[0]
        for step, out_ref in zip(steps, out_refs):
            head = head_of(place_ref[0] ^ step, lane, head_axis)
            heads.append(head)
            first = pl.multiple_of(head * size, size)
            for which, ref in enumerate((k_ref, v_ref)):
                move = pltpu.make_async_copy(
                    ref.at[:, pl.ds(first, size)],
                    out_ref.at[pl.ds(which * rows, rows), :],
                    sem.at[len(moves)],
                )
                move.start()
                moves.append(move)
        rates = r_ref[...].astype(jnp.float32)
        head_id = lax.broadcasted_iota(jnp.int32, rates.shape, 0)
        for head, out_ref in zip(heads, out_refs):
            row = jnp.sum(jnp.where(head_id == head, rates, 0.0), axis=0, keepdims=True)
            wide = jnp.broadcast_to(row, (RATE_ROWS, rows)).astype(jnp.bfloat16)
            for first in range(0, size, rows):
                out_ref[2 * rows :, first : first + rows] = wide
        if loaded:
            for which, (load, ref) in enumerate(zip(loads, w_refs)):
                load.wait()
                for head in range(ref.shape[1]):
                    w_out_ref[head, which] = ref[:, head, :]
        for move in moves:
            move.wait()

    out_shape = [pltpu.VMEM((2 * rows + RATE_ROWS, size), jnp.bfloat16)] * count
    scratch = [pltpu.SemaphoreType.DMA((count * 2,))]
    if loaded:
        piece, local, _ = weights[0].shape
        out_shape += [pltpu.HBM((local, loaded, piece, size), jnp.bfloat16)]
        scratch += [pltpu.VMEM(w.shape, w.dtype) for w in weights]
        scratch += [pltpu.SemaphoreType.DMA((loaded,))]
    return pl.pallas_call(
        kernel,
        in_specs=[SMEM, ANY, ANY, VMEM] + [ANY] * loaded,
        out_specs=[VMEM] * len(out_shape),
        out_shape=out_shape,
        scratch_shapes=scratch,
        compiler_params=params(),
        name="pack",
    )(place, *[in_hbm(x) for x in (key_rows, value_rows, rates_t, *weights)])


def pack_queries(place, queries, lane, head_axis):
    rows, width = queries.shape
    size = width // HEADS

    def kernel(place_ref, q_ref, *refs):
        out_refs, sem = refs[:HEADS], refs[HEADS]
        moves = []
        for step, out_ref in enumerate(out_refs):
            head = head_of(place_ref[0] ^ step, lane, head_axis)
            first = pl.multiple_of(head * size, size)
            move = pltpu.make_async_copy(q_ref.at[:, pl.ds(first, size)], out_ref, sem.at[step])
            move.start()
            moves.append(move)
        for move in moves:
            move.wait()

    return pl.pallas_call(
        kernel,
        in_specs=[SMEM, ANY],
        out_specs=[VMEM] * HEADS,
        out_shape=[pltpu.VMEM((rows, size), jnp.bfloat16)] * HEADS,
        scratch_shapes=[pltpu.SemaphoreType.DMA((HEADS,))],
        compiler_params=params(),
        name="pack_queries",
    )(place, in_hbm(queries))


def unpack_columns(place, back, lane, head_axis):
    rows, size = back[0].shape

    def kernel(place_ref, *refs):
        back_refs, out_ref, sem = refs[:HEADS], refs[HEADS], refs[HEADS + 1]
        moves = []
        for step, ref in enumerate(back_refs):
            head = head_of(place_ref[0] ^ step, lane, head_axis)
            first = pl.multiple_of(head * size, size)
            move = pltpu.make_async_copy(ref, out_ref.at[:, pl.ds(first, size)], sem.at[step])
            move.start()
            moves.append(move)
        for move in moves:
            move.wait()

    return pl.pallas_call(
        kernel,
        in_specs=[SMEM] + [VMEM] * HEADS,
        out_specs=ANY,
        out_shape=pltpu.HBM((rows, HEADS * size), back[0].dtype),
        scratch_shapes=[pltpu.SemaphoreType.DMA((HEADS,))],
        compiler_params=params(),
        name="unpack_columns",
    )(place, *[in_vmem(x) for x in back])


def place_pieces(spot_ref, piece_refs, out_ref, outer, lane, inner):
    if len(piece_refs) == 1:
        out_ref[...] = piece_refs[0][...]
        return
    piece = piece_refs[0].shape[2]
    a, c = spot_ref[0], spot_ref[1]
    spots = [(a, c), (outer - 1 - a, c), (a, inner - 1 - c), (outer - 1 - a, inner - 1 - c)]
    for (at_a, at_c), ref in zip(spots, piece_refs):
        for l in range(lane):
            first = pl.multiple_of(((at_a * lane + l) * inner + at_c) * piece, piece)
            for which in range(ref.shape[1]):
                out_ref[which, pl.ds(first, piece), :] = ref[l, which]


def split_pieces(own):
    lane, _, piece, size = own.shape

    def kernel(own_ref, first_ref, last_ref):
        for l in range(lane):
            first_ref[l] = own_ref[l, :2]
            last_ref[l] = own_ref[l, 2:]

    return pl.pallas_call(
        kernel,
        in_specs=[VMEM],
        out_specs=[VMEM] * 2,
        out_shape=[
            pltpu.VMEM((lane, 2, piece, size), own.dtype),
            pltpu.VMEM((lane, 1, piece, size), own.dtype),
        ],
        compiler_params=params(),
        name="split_pieces",
    )(in_vmem(own))


def total_of(left_ref, right_ref, part):
    return lax.dot_general(
        left_ref[part], right_ref[...], (((0,), (0,)), ((), ())), preferred_element_type=jnp.float32
    )


def down_gradient(spot, place, received, pieces, rows, outer, lane, inner, per_run):
    blocks = len(received)
    size = received[0].shape[1]
    runs = blocks // per_run
    half = size // inner
    count = blocks * rows
    group = 2 if blocks % 2 == 0 else 1
    span = group * rows

    def kernel(spot_ref, place_ref, *refs):
        kv_refs, refs = refs[:blocks], refs[blocks:]
        piece_refs, refs = refs[: len(pieces)], refs[len(pieces) :]
        keep_ref, send_ref, tail_ref, last_ref, w_ref, kn_ref, tgt_ref, gf_ref, uf_ref = refs[:9]
        hid_ref, all_ref = refs[9:]
        place_pieces(spot_ref, piece_refs, w_ref, outer, lane, inner)
        for g in range(blocks // group):
            here = slice(g * span, (g + 1) * span)
            mine = range(g * group, (g + 1) * group)

            for b in mine:
                row = kv_refs[b][2 * rows : 2 * rows + 1, :rows].astype(jnp.float32)
                rate_columns = -jnp.broadcast_to(row, (rows, rows)).T
                for first in range(0, rows, STRIP):
                    there = slice(b * rows + first, b * rows + first + STRIP)
                    key_norm = rms_rows(kv_refs[b][first : first + STRIP, :])
                    for part in range(inner):
                        kn_ref[part, there, :] = key_norm[:, part * half : (part + 1) * half]
                    values = kv_refs[b][rows + first : rows + first + STRIP, :].astype(jnp.float32)
                    strip_rates = jnp.concatenate(
                        [rate_columns[first : first + STRIP, :]] * (size // rows), axis=1
                    )
                    tgt_ref[there, :] = (strip_rates * values).astype(jnp.bfloat16)
            keys = jnp.concatenate([kn_ref[part, here, :] for part in range(inner)], axis=1)
            gf_ref[here, :] = jnp.dot(keys, w_ref[0], preferred_element_type=jnp.float32)
            uf_ref[here, :] = jnp.dot(keys, w_ref[1], preferred_element_type=jnp.float32)
            for first in range(g * span, (g + 1) * span, STRIP):
                there = slice(first, first + STRIP)
                gate_pre, up_pre = gf_ref[there, :], uf_ref[there, :]
                sigma_gate = jax.nn.sigmoid(gate_pre)
                silu_gate = gate_pre * sigma_gate
                hidden = (silu_gate * up_pre).astype(jnp.bfloat16)
                for part in range(inner):
                    hid_ref[part, there, :] = hidden[:, part * half : (part + 1) * half]
                gf_ref[there, :] = up_pre * sigma_gate * (1.0 + gate_pre * (1.0 - sigma_gate))
                uf_ref[there, :] = silu_gate
        own = spot_ref[1]
        send_ref[0] = total_of(hid_ref, tgt_ref, inner - 1 - own).astype(jnp.bfloat16)
        keep_ref[0] = total_of(hid_ref, tgt_ref, own)
        for step, ref in enumerate(kv_refs):
            block = place_ref[0] ^ step
            for which in range(2):
                end = (which + 1) * rows
                all_ref[block, which * WINDOW : (which + 1) * WINDOW, :] = ref[end - WINDOW : end, :]
        for run in range(runs):
            tail_ref[run] = all_ref[(run + 1) * per_run - 1]
        last_ref[0] = all_ref[blocks - 1]

    return pl.pallas_call(
        kernel,
        in_specs=[SMEM] * 2 + [VMEM] * (blocks + len(pieces)),
        out_specs=[VMEM] * 9,
        out_shape=[
            pltpu.VMEM((1, half, size), jnp.float32),
            pltpu.VMEM((1, half, size), jnp.bfloat16),
            pltpu.VMEM((runs, 2 * WINDOW, size), jnp.bfloat16),
            pltpu.VMEM((1, 2 * WINDOW, size), jnp.bfloat16),
            pltpu.VMEM((2, size, size), jnp.bfloat16),
            pltpu.VMEM((inner, count, half), jnp.bfloat16),
            pltpu.VMEM((count, size), jnp.bfloat16),
            pltpu.VMEM((count, size), jnp.float32),
            pltpu.VMEM((count, size), jnp.float32),
        ],
        scratch_shapes=[
            pltpu.VMEM((inner, count, half), jnp.bfloat16),
            pltpu.VMEM((blocks, 2 * WINDOW, size), jnp.bfloat16),
        ],
        compiler_params=params(14),
        cost_estimate=cost(4),
        name="down_gradient",
    )(spot, place, *[in_vmem(r) for r in received], *[in_vmem(p) for p in pieces])


def other_gradients(spot, pieces, key_norm, target, gate_factor, up_factor, outer, lane):
    inner, count, half = key_norm.shape
    size = target.shape[1]
    span = count // 4

    def kernel(spot_ref, *refs):
        piece_refs, refs = refs[: len(pieces)], refs[len(pieces) :]
        kn_ref, tgt_ref, gf_ref, uf_ref, keep_ref, send_ref, w_ref, gg_ref, ug_ref, hg_ref = refs
        place_pieces(spot_ref, piece_refs, w_ref, outer, lane, inner)
        for first in range(0, count, span):
            here = slice(first, first + span)
            hg_ref[here, :] = lax.dot_general(
                tgt_ref[here, :],
                w_ref[0],
                (((1,), (1,)), ((), ())),
                preferred_element_type=jnp.float32,
            )
            for strip in range(first, first + span, STRIP):
                there = slice(strip, strip + STRIP)
                hidden_grad = hg_ref[there, :]
                gg_ref[there, :] = (hidden_grad * gf_ref[there, :]).astype(jnp.bfloat16)
                ug_ref[there, :] = (hidden_grad * uf_ref[there, :]).astype(jnp.bfloat16)
        own = spot_ref[1]
        for which, right_ref in enumerate((gg_ref, ug_ref)):
            send_ref[which] = total_of(kn_ref, right_ref, inner - 1 - own).astype(jnp.bfloat16)
            keep_ref[which] = total_of(kn_ref, right_ref, own)

    return pl.pallas_call(
        kernel,
        in_specs=[SMEM] + [VMEM] * (len(pieces) + 4),
        out_specs=[VMEM] * 3,
        out_shape=[
            pltpu.VMEM((2, half, size), jnp.float32),
            pltpu.VMEM((2, half, size), jnp.bfloat16),
            pltpu.VMEM((1, size, size), jnp.bfloat16),
        ],
        scratch_shapes=[pltpu.VMEM((count, size), jnp.bfloat16)] * 2
        + [pltpu.VMEM((count, size), jnp.float32)],
        compiler_params=params(10),
        cost_estimate=cost(3),
        name="other_gradients",
    )(
        spot,
        *[in_vmem(p) for p in pieces],
        *[in_vmem(x) for x in (key_norm, target, gate_factor, up_factor)],
    )


def combine(keep, got):
    def kernel(keep_ref, got_ref, out_ref):
        out_ref[...] = (keep_ref[...] + got_ref[...].astype(jnp.float32)).astype(jnp.bfloat16)

    return pl.pallas_call(
        kernel,
        in_specs=[VMEM, VMEM],
        out_specs=VMEM,
        out_shape=pltpu.VMEM(keep.shape, jnp.bfloat16),
        compiler_params=params(),
        name="combine",
    )(in_vmem(keep), in_vmem(got))


def attention(spot, place, queries, received, around, from_outer, old_first, old_last, per_run):
    blocks = len(queries)
    rows, width = queries[0].shape
    span = 2 * WINDOW

    def kernel(spot_ref, place_ref, w_ref, w_last_ref, around_ref, outer_ref, *refs):
        q_refs, kv_refs, refs = refs[:blocks], refs[blocks : 2 * blocks], refs[2 * blocks :]
        att_ref, qn_ref, norm_ref, kv_ref, q_ref = refs
        for step in range(blocks):
            kv_ref[place_ref[0] ^ step] = kv_refs[step][: 2 * rows, :]
            q_ref[place_ref[0] ^ step] = q_refs[step][...]
        for which in range(3):
            for first in range(0, width, HEAD_DIM):
                source, index = (w_ref, which) if which < 2 else (w_last_ref, 0)
                previous = source[index, first : first + HEAD_DIM, :].astype(jnp.float32)
                norm = jnp.sqrt(jnp.mean(previous * previous, axis=1, keepdims=True))
                norm_ref[which, first : first + HEAD_DIM, :] = jnp.broadcast_to(
                    norm, (HEAD_DIM, HEAD_DIM)
                )
        on_first = jnp.where(spot_ref[1] == 0, 1, 0)
        begins = jnp.where(spot_ref[0] == 0, on_first, 0)
        row_id = lax.broadcasted_iota(jnp.int32, (WINDOW, span), 0)
        key_id = lax.broadcasted_iota(jnp.int32, (WINDOW, span), 1)
        allowed = (key_id <= row_id + WINDOW) & (key_id > row_id)
        bias = jnp.where(allowed, 0.0, -1e30)
        first_key = jnp.where(begins == 1, WINDOW, 0)
        first_bias = jnp.where(allowed & (key_id >= first_key), 0.0, -1e30)
        for b in range(blocks):
            qn_ref[b] = rms_rows(q_ref[b])
            pieces = [
                (part, first)
                for part in range(rows // WINDOW)
                for first in range(0, width, HEAD_DIM)
            ]

            def keys_or_values(which, part, first):
                columns = slice(first, first + HEAD_DIM)
                end = which * rows + (part + 1) * WINDOW
                if part:
                    return kv_ref[b, end - span : end, columns]
                before = slice(which * WINDOW, (which + 1) * WINDOW)
                if b % per_run:
                    after = (which + 1) * rows
                    tail = kv_ref[b - 1, after - WINDOW : after, columns]
                elif b:
                    tail = around_ref[b // per_run - on_first, before, columns]
                else:
                    tail = jnp.where(
                        on_first == 1, outer_ref[0, before, columns], around_ref[0, before, columns]
                    )
                return jnp.concatenate([tail, kv_ref[b, end - WINDOW : end, columns]], axis=0)

            masked = []
            for part, first in pieces:
                scores = lax.dot_general(
                    q_ref[b, part * WINDOW : (part + 1) * WINDOW, first : first + HEAD_DIM],
                    keys_or_values(0, part, first),
                    (((1,), (1,)), ((), ())),
                    preferred_element_type=jnp.float32,
                )
                masked.append(
                    scores * (1.0 / math.sqrt(HEAD_DIM)) + (bias if b or part else first_bias)
                )
            masked = jnp.concatenate(masked, axis=0)
            maximum = jnp.max(masked, axis=1, keepdims=True)
            exp_scores = jnp.exp(masked - maximum)
            scale = 1.0 / jnp.sum(exp_scores, axis=1, keepdims=True)
            weights = exp_scores.astype(jnp.bfloat16)
            for i, (part, first) in enumerate(pieces):
                here = slice(i * WINDOW, (i + 1) * WINDOW)
                mixed = jnp.dot(
                    weights[here],
                    keys_or_values(1, part, first),
                    preferred_element_type=jnp.float32,
                )
                att_ref[b, part * WINDOW : (part + 1) * WINDOW, first : first + HEAD_DIM] = (
                    mixed * scale[here]
                )

    return pl.pallas_call(
        kernel,
        in_specs=[SMEM] * 2 + [VMEM] * (4 + 2 * blocks),
        out_specs=[VMEM] * 3,
        out_shape=[
            pltpu.VMEM((blocks, rows, width), jnp.float32),
            pltpu.VMEM((blocks, rows, width), jnp.bfloat16),
            pltpu.VMEM((3, width, HEAD_DIM), jnp.float32),
        ],
        scratch_shapes=[
            pltpu.VMEM((blocks, 2 * rows, width), jnp.bfloat16),
            pltpu.VMEM((blocks, rows, width), jnp.bfloat16),
        ],
        compiler_params=params(10),
        cost_estimate=cost(6),
        name="attention",
    )(
        spot,
        place,
        in_vmem(old_first),
        in_vmem(old_last),
        in_vmem(around),
        in_vmem(from_outer),
        *[in_vmem(q) for q in queries],
        *[in_vmem(r) for r in received],
    )


def update_and_apply(spot, place, old_first, old_last, norms, first, last, query_norm, attended):
    sums = first + last
    blocks, rows, size = query_norm.shape
    halves = len(first) // 2
    half = size // halves
    group = 2 if blocks % 2 == 0 else 1

    def kernel(spot_ref, place_ref, w_ref, w_last_ref, norm_ref, *refs):
        sum_refs, refs = refs[: len(sums)], refs[len(sums) :]
        q_ref, a_ref, out_refs = refs[0], refs[1], refs[2:-6]
        total_ref, new_ref, gate_ref, up_ref, hid_ref, fast_ref = refs[-6:]
        squares = jnp.zeros((8, size), jnp.float32)
        for part in range(halves):
            place = spot_ref[1] if part == 0 else halves - 1 - spot_ref[1]
            for which in range(3):
                begin, index = (2 * part, which) if which < 2 else (2 * halves + 2 * part, 0)
                for row in range(0, half, STRIP):
                    there = slice(row, row + STRIP)
                    total = sum_refs[begin][index, there, :].astype(jnp.float32) + sum_refs[
                        begin + 1
                    ][index, there, :].astype(jnp.float32)
                    total_ref[place, which, there, :] = total
                    squares = squares + jnp.sum(
                        (total * total).reshape(STRIP // 8, 8, size), axis=0
                    )
        norm_scale = lax.rsqrt(
            jnp.sum(squares, axis=(0, 1), keepdims=True) / (3 * size * size) + NORM_EPS
        )
        scale = STEP_SIZE * norm_scale
        for part in range(halves):
            for which in range(3):
                source, index = (w_ref, which) if which < 2 else (w_last_ref, 0)
                for row in range(0, half, STRIP):
                    here = slice(part * half + row, part * half + row + STRIP)
                    previous = source[index, here, :].astype(jnp.float32)
                    stepped = previous - scale * total_ref[part, which, row : row + STRIP, :]
                    factor = norm_ref[which, here, 0:1] * lax.rsqrt(
                        jnp.mean(stepped * stepped, axis=1, keepdims=True) + NORM_EPS
                    )
                    new_ref[which, here, :] = (stepped * factor).astype(jnp.bfloat16)
        for g in range(blocks // group):
            steps = range(g * group, (g + 1) * group)
            mine = [place_ref[0] ^ step for step in steps]
            query = jnp.concatenate([q_ref[b] for b in mine], axis=0)
            here = slice(g * group * rows, (g + 1) * group * rows)
            gate_ref[here, :] = jnp.dot(query, new_ref[0], preferred_element_type=jnp.float32)
            up_ref[here, :] = jnp.dot(query, new_ref[1], preferred_element_type=jnp.float32)
            for row in range(g * group * rows, (g + 1) * group * rows, STRIP):
                there = slice(row, row + STRIP)
                query_gate = gate_ref[there, :]
                hid_ref[there, :] = (
                    query_gate * jax.nn.sigmoid(query_gate) * up_ref[there, :]
                ).astype(jnp.bfloat16)
            fast_ref[here, :] = jnp.dot(
                hid_ref[here, :], new_ref[2], preferred_element_type=jnp.float32
            )
            for i, (step, b) in enumerate(zip(steps, mine)):
                for row in range(0, rows, STRIP):
                    there = slice(row, row + STRIP)
                    start = (g * group + i) * rows + row
                    fast = fast_ref[start : start + STRIP, :].astype(jnp.bfloat16)
                    out_refs[step][there, :] = (
                        a_ref[b, there, :] + fast.astype(jnp.float32)
                    ).astype(jnp.bfloat16)

    return pl.pallas_call(
        kernel,
        in_specs=[SMEM] * 2 + [VMEM] * (len(sums) + 5),
        out_specs=[VMEM] * blocks,
        out_shape=[pltpu.VMEM((rows, size), jnp.bfloat16)] * blocks,
        scratch_shapes=[
            pltpu.VMEM((halves, 3, half, size), jnp.float32),
            pltpu.VMEM((3, size, size), jnp.bfloat16),
            pltpu.VMEM((blocks * rows, size), jnp.float32),
            pltpu.VMEM((blocks * rows, size), jnp.float32),
            pltpu.VMEM((blocks * rows, size), jnp.bfloat16),
            pltpu.VMEM((blocks * rows, size), jnp.float32),
        ],
        compiler_params=params(20),
        cost_estimate=cost(6),
        name="update_and_apply",
    )(
        spot,
        place,
        in_vmem(old_first),
        in_vmem(old_last),
        in_vmem(norms),
        *[in_vmem(s) for s in sums],
        in_vmem(query_norm),
        in_vmem(attended),
    )


def gather_rows(mine, axis, count, index, order_axis):
    if count & (count - 1):
        return lax.all_gather(mine, axis, axis=order_axis, tiled=True)
    stride = 1
    while stride < count:
        theirs = lax.ppermute(mine, axis, swap_pairs(count, stride))
        low = (index // stride) % 2 == 0
        mine = jnp.concatenate(
            [jnp.where(low, mine, theirs), jnp.where(low, theirs, mine)], order_axis
        )
        stride *= 2
    return mine


def make_shards(outer, lane, inner, head_axis):
    group = ("lane", "head")

    def shards(queries, key_rows, value_rows, step_rates, w_gate, w_up, w_down):
        rows, width = queries.shape
        size = width // HEADS
        a = lax.axis_index("outer")
        c = lax.axis_index("inner")
        spot = jnp.stack([a, c]).astype(jnp.int32)
        place = jnp.reshape(lax.axis_index(group), (1,)).astype(jnp.int32)
        spot, place, w_gate = lax.optimization_barrier((spot, place, w_gate))

        rates_t = jnp.transpose(step_rates)
        begin = KEY_STEPS[:1]
        rest = tuple(step for step in range(HEADS) if step not in begin)
        *packed, own = pack(
            place, key_rows, value_rows, rates_t, begin, (w_gate, w_up, w_down), lane, head_axis
        )
        packed += pack(place, key_rows, value_rows, rates_t, rest, (), lane, head_axis)
        packed = dict(zip(begin + rest, packed))
        if lane > 1:
            own = lax.all_to_all(own, "lane", split_axis=0, concat_axis=0, tiled=True)

        def exchange(chunks):
            got = [chunks[0]]
            for step in range(1, HEADS):
                got.append(lax.ppermute(chunks[step], group, swap_pairs(HEADS, step)))
            return got

        kv = exchange(packed)
        qs = pack_queries(place, queries, lane, head_axis)
        qs = exchange(qs)

        if outer == 2 and inner == 2:
            first_pieces, last_pieces = ([part] for part in split_pieces(own))
            for pieces in (first_pieces, last_pieces):
                pieces.append(lax.ppermute(pieces[0], "outer", swap_pairs(outer, 1)))
                pieces.append(lax.ppermute(pieces[0], "inner", swap_pairs(inner, 1)))
                pieces.append(lax.ppermute(pieces[1], "inner", swap_pairs(inner, 1)))
        else:
            old = gather_rows(own[None], "outer", outer, a, 0)[:, :, None]
            old = gather_rows(old, "inner", inner, c, 2)
            old = jnp.transpose(old, (3, 0, 1, 2, 4, 5)).reshape(3, size, size)
            first_pieces, last_pieces = [old[:2]], [old[2:]]

        def begin_sum(keep, send):
            half = keep.astype(jnp.bfloat16)
            if inner > 1:
                got = lax.ppermute(send, "inner", swap_pairs(inner, 1))
                half = combine(keep, got)
            mine, theirs = half, jnp.zeros_like(half)
            if outer & (outer - 1):
                return lax.psum(half, "outer"), theirs
            stride = 1
            while stride < outer:
                if stride > 1:
                    mine = (mine.astype(jnp.float32) + theirs.astype(jnp.float32)).astype(
                        jnp.bfloat16
                    )
                theirs = lax.ppermute(mine, "outer", swap_pairs(outer, stride))
                stride *= 2
            return mine, theirs

        def share(value):
            return lax.ppermute(value, "inner", swap_pairs(inner, 1))

        keep, send, tails, last, old_first, *rest = down_gradient(
            spot, place, kv, first_pieces, rows, outer, lane, inner, head_axis
        )
        last_sums = list(begin_sum(keep, send))
        keep, send, old_last = other_gradients(spot, last_pieces, *rest, outer, lane)
        first_sums = list(begin_sum(keep, send))
        around = tails
        if inner > 1:
            around = lax.ppermute(tails, "inner", [(i, (i + 1) % inner) for i in range(inner)])
        pairs = [
            (i * inner + inner - 1, (i + 1) * inner) for i in range(outer - 1)
        ]
        from_outer = lax.ppermute(last, ("outer", "inner"), pairs) if pairs else last
        attended, query_norm, norms = attention(
            spot, place, qs, kv, around, from_outer, old_first, old_last, head_axis
        )

        first_sums[1], attended, query_norm, norms = lax.optimization_barrier(
            (first_sums[1], attended, query_norm, norms)
        )
        if inner > 1:
            last_sums += [share(last_sums[0]), share(last_sums[1])]
            first_sums += [share(first_sums[0]), share(first_sums[1])]

        out = update_and_apply(
            spot, place, old_first, old_last, norms, first_sums, last_sums, query_norm, attended
        )
        return unpack_columns(place, exchange(out), lane, head_axis)

    return shards


def solution(mesh):
    seq, head_axis = mesh.shape["seq"], mesh.shape["head"]
    lane = HEADS // head_axis
    inner = 2 if (seq // lane) % 2 == 0 else 1
    outer = seq // lane // inner
    names = ("outer", "lane", "inner", "head")
    split = Mesh(mesh.devices.reshape(outer, lane, inner, head_axis), names)
    rows = P(names, None)
    weights = P(names[:3], names[3], None)
    shards = make_shards(outer, lane, inner, head_axis)

    return jax.shard_map(
        shards,
        mesh=split,
        in_specs=(rows, rows, rows, rows, weights, weights, weights),
        out_specs=rows,
        check_vma=False,
    )
```
